256 devices in a mesh: grp: 2 (over core), gx: 32 (over y, z), gy: 4 (over x).
Axes of the slice: x: 4, y: 4, z: 8, core: 2. Of those that a mesh axis runs over, the one named last changes fastest.
Arguments:
- coarse_ez: float32 [2048, 1024], P('gx', ('grp', 'gy')), may hold values from -6 to 6
- coarse_hx: float32 [2048, 1024], P('gx', ('grp', 'gy')), may hold values from -6 to 6
- coarse_hy: float32 [2048, 1024], P('gx', ('grp', 'gy')), may hold values from -6 to 6
- coarse_ids: int32 [2048, 1024], P('gx', ('grp', 'gy')), may hold values from 0 to 7
- mat_eps: float32 [8], replicated, may hold values from 1 to 12
- mat_sig: float32 [8], replicated, may hold values from 0 to 0.5
- fine_ez: float32 [32, 8, 32, 2304], P(None, ('grp', 'gy'), 'gx'), may hold values from -6 to 6
- fine_hx: float32 [32, 8, 32, 2304], P(None, ('grp', 'gy'), 'gx'), may hold values from -6 to 6
- fine_hy: float32 [32, 8, 32, 2304], P(None, ('grp', 'gy'), 'gx'), may hold values from -6 to 6
- fine_ids: int32 [32, 8, 32, 2304], P(None, ('grp', 'gy'), 'gx'), may hold values from 0 to 7
- boxes: int32 [32, 8, 32, 4], P('gx', ('grp', 'gy')), may hold values from 1 to 14, as said below
- src_cells: int32 [4], replicated, may hold values from 0 to 2097151
- src_wave: float32 [3, 4], replicated, may hold values from -6 to 6
- rcv_cells: int32 [128], replicated, may hold values from 0 to 2097151
Outputs:
- end_ez: float32 [2048, 1024], P('gx', ('grp', 'gy'))
- end_hx: float32 [2048, 1024], P('gx', ('grp', 'gy'))
- end_hy: float32 [2048, 1024], P('gx', ('grp', 'gy'))
- end_fine_ez: float32 [32, 8, 32, 2304], P(None, ('grp', 'gy'), 'gx')
- end_fine_hx: float32 [32, 8, 32, 2304], P(None, ('grp', 'gy'), 'gx')
- end_fine_hy: float32 [32, 8, 32, 2304], P(None, ('grp', 'gy'), 'gx')
- traces: float32 [3, 128], replicated
The draws below stay inside these ranges and needn't reach their ends.
Inputs may be any that keep to these rules, and one draw needn't show every extreme that they name: `boxes`: each box lies one cell or more inside its tile: corner + size <= 15; sizes are 4 to 14, drawn independently for every subgrid.
All inputs are finite; a program needn't handle non-finite values.
Results may differ from the reference program's by a relative error of at most 0.00011.
Values sent between devices are 32-bit elements; how exact they have to be, the bound alone decides.
A program may use at most 64 MiB of HBM per device.

```python
import math
import jax
import jax.numpy as jnp

TILE = 16
FINE = 48
CAP = 32
STEPS = 3
NMAT = 8
NSRC = 4
NRCV = 128
BLOCKS_X = 32
BLOCKS_Y = 8
NX = 2048
NY = 1024


def draw_boxes(key, part):
    first, second, third, fourth = jax.random.split(jax.random.fold_in(key, 17), 4)
    shape = (BLOCKS_X, BLOCKS_Y, CAP)
    size_i = jax.random.randint(first, shape, 4, TILE - 1)
    size_j = jax.random.randint(second, shape, 4, TILE - 1)
    corner_i = jax.random.randint(third, shape, 1, TILE - size_i)
    corner_j = jax.random.randint(fourth, shape, 1, TILE - size_j)
    return jnp.stack([corner_i, corner_j, size_i, size_j], -1).astype(jnp.int32)


def plant(entries, stream_key, low, largest):
    shape = entries.shape
    index_at = [jax.random.randint(jax.random.fold_in(stream_key, axis), (), 0, shape[axis]) for axis in range(len(shape))]
    entries = entries.at[tuple(index_at)].set(low)
    longest = shape.index(max(shape))
    index_at[longest] = (index_at[longest] + 1) % shape[longest]
    return entries.at[tuple(index_at)].set(largest)


def block_levels(key, dims, shards, least, top_value):
    level = 1.0
    for axis_at, shards_of in shards:
        steps = jax.random.uniform(jax.random.fold_in(jax.random.fold_in(key, 6), axis_at), (shards_of,), jnp.float32, least / len(shards), top_value / len(shards))
        level = level * jnp.repeat(jnp.exp(steps), dims[axis_at] // shards_of).reshape((-1,) + (1,) * (len(dims) - 1 - axis_at))
    return level


def bell_draw(rng, dims, spread, reach, cuts=(), kind=jnp.bfloat16):
    entries = spread * jax.random.normal(rng, dims, jnp.float32)
    if cuts:
        entries = entries * block_levels(rng, dims, cuts, -0.22, 0.18)
    return jnp.clip(entries, -reach, reach).astype(kind)


def setup_inputs(seed: int = 0) -> dict:
    splits = jax.random.split(jax.random.key(seed), 15)
    return {
        "coarse_ez": bell_draw(splits[0], (NX, NY), 1.0, 6.0, ((0, 32), (1, 8)), jnp.float32),
        "coarse_hx": bell_draw(splits[1], (NX, NY), 1.0, 6.0, ((0, 32), (1, 8)), jnp.float32),
        "coarse_hy": bell_draw(splits[2], (NX, NY), 1.0, 6.0, ((0, 32), (1, 8)), jnp.float32),
        "coarse_ids": plant(jax.random.randint(splits[3], (NX, NY), 0, NMAT), jax.random.fold_in(splits[3], 1), 0, NMAT - 1).astype(jnp.int32),
        "mat_eps": jnp.clip(jnp.exp(jax.random.uniform(splits[4], (NMAT,), jnp.float32, math.log(1.0), math.log(12.0))), 1.0, 12.0),
        "mat_sig": jnp.clip(jax.random.uniform(splits[5], (NMAT,), jnp.float32, 0.0, 0.5), 0.0, 0.5),
        "fine_ez": bell_draw(splits[6], (BLOCKS_X, BLOCKS_Y, CAP, FINE * FINE), 1.0, 6.0, ((1, 8), (2, 32)), jnp.float32),
        "fine_hx": bell_draw(splits[7], (BLOCKS_X, BLOCKS_Y, CAP, FINE * FINE), 1.0, 6.0, ((1, 8), (2, 32)), jnp.float32),
        "fine_hy": bell_draw(splits[8], (BLOCKS_X, BLOCKS_Y, CAP, FINE * FINE), 1.0, 6.0, ((1, 8), (2, 32)), jnp.float32),
        "fine_ids": plant(jax.random.randint(splits[9], (BLOCKS_X, BLOCKS_Y, CAP, FINE * FINE), 0, NMAT), jax.random.fold_in(splits[9], 1), 0, NMAT - 1).astype(jnp.int32),
        "boxes": draw_boxes(jax.random.fold_in(splits[14], 71), 0),
        "src_cells": plant(jax.random.randint(splits[11], (NSRC,), 0, NX * NY), jax.random.fold_in(splits[11], 1), 0, (NX * NY) - 1).astype(jnp.int32),
        "src_wave": bell_draw(splits[12], (STEPS, NSRC), 1.0, 6.0, (), jnp.float32),
        "rcv_cells": plant(jax.random.randint(splits[13], (NRCV,), 0, NX * NY), jax.random.fold_in(splits[13], 1), 0, (NX * NY) - 1).astype(jnp.int32),
    }


COURANT = 0.5
HCOEF = 0.5


def coefficients(ids, eps_table, sig_table, ratio):
    damp = jnp.zeros(ids.shape, jnp.float32)
    gain = jnp.zeros(ids.shape, jnp.float32)
    for material in range(eps_table.shape[0]):
        loss = sig_table[material] / (eps_table[material] * ratio)
        hit = ids == material
        damp = jnp.where(hit, (1.0 - loss) / (1.0 + loss), damp)
        gain = jnp.where(hit, COURANT / (eps_table[material] * (1.0 + loss)), gain)
    return damp, gain


def box_masks(boxes, cells, scale):
    coarse_of = jnp.arange(cells, dtype=jnp.int32) // scale
    low_i = boxes[..., 0:1]
    low_j = boxes[..., 1:2]
    high_i = low_i + boxes[..., 2:3]
    high_j = low_j + boxes[..., 3:4]
    rows_in = (coarse_of >= low_i) & (coarse_of < high_i)
    cols_in = (coarse_of >= low_j) & (coarse_of < high_j)
    rows_mid = (coarse_of > low_i) & (coarse_of < high_i - 1)
    cols_mid = (coarse_of > low_j) & (coarse_of < high_j - 1)
    inbox = rows_in[..., :, None] & cols_in[..., None, :]
    middle = rows_mid[..., :, None] & cols_mid[..., None, :]
    return inbox, middle


def flat_masks(boxes):
    width = TILE * 3
    index = jnp.arange(width * width, dtype=jnp.int32)
    coarse_i = index // width // 3
    coarse_j = index % width // 3
    low_i = boxes[..., 0:1]
    low_j = boxes[..., 1:2]
    high_i = low_i + boxes[..., 2:3]
    high_j = low_j + boxes[..., 3:4]
    inbox = (coarse_i >= low_i) & (coarse_i < high_i) & (coarse_j >= low_j) & (coarse_j < high_j)
    middle = (coarse_i > low_i) & (coarse_i < high_i - 1) & (coarse_j > low_j) & (coarse_j < high_j - 1)
    return inbox, middle


def to_tiles(field, blocks_x, blocks_y):
    rows, cols = field.shape
    along_x = rows // blocks_x // TILE
    along_y = cols // blocks_y // TILE
    shaped = field.reshape(blocks_x, along_x, TILE, blocks_y, along_y, TILE)
    shaped = shaped.transpose(0, 3, 1, 4, 2, 5)
    return shaped.reshape(blocks_x, blocks_y, along_x * along_y, TILE, TILE)


def from_tiles(tiles, block_rows, block_cols):
    blocks_x, blocks_y = tiles.shape[0], tiles.shape[1]
    along_x = block_rows // TILE
    along_y = block_cols // TILE
    shaped = tiles.reshape(blocks_x, blocks_y, along_x, along_y, TILE, TILE)
    shaped = shaped.transpose(0, 2, 4, 1, 3, 5)
    return shaped.reshape(blocks_x * block_rows, blocks_y * block_cols)


def pad_last(array, before, after):
    widths = [(0, 0)] * (array.ndim - 1) + [(before, after)]
    return jnp.pad(array, widths)


def fine_substep(fine_ez, fine_hx, fine_hy, damp, gain, inbox, middle, border, cycle_value):
    width = TILE * 3
    column = jnp.arange(width * width, dtype=jnp.int32) % width
    ez_next_col = jnp.where(column < width - 1, pad_last(fine_ez[..., 1:], 0, 1), 0.0)
    ez_next_row = pad_last(fine_ez[..., width:], 0, width)
    fine_hx = jnp.where(inbox, fine_hx - HCOEF * (ez_next_col - fine_ez), 0.0)
    fine_hy = jnp.where(inbox, fine_hy + HCOEF * (ez_next_row - fine_ez), 0.0)
    hy_prev = pad_last(fine_hy[..., :-width], width, 0)
    hx_prev = jnp.where(column > 0, pad_last(fine_hx[..., :-1], 1, 0), 0.0)
    curl = (fine_hy - hy_prev) - (fine_hx - hx_prev)
    inner = damp * fine_ez + gain * curl
    fine_ez = jnp.where(middle, inner, jnp.where(border, cycle_value, 0.0))
    return fine_ez, fine_hx, fine_hy


def upsample(tiles):
    lead = tiles.shape[:-2]
    wide = jnp.repeat(jnp.repeat(tiles, 3, axis=-2), 3, axis=-1)
    return wide.reshape(lead + (TILE * TILE * 9,))


def cell_means(fine_ez):
    lead = fine_ez.shape[:-1]
    shaped = fine_ez.reshape(lead + (TILE, 3, TILE, 3))
    return jnp.sum(shaped, axis=(-3, -1)) / 9.0


def fine_round(fine_ez, fine_hx, fine_hy, damp, gain, inbox, middle, border, old_tiles, new_tiles):
    for sub in range(1, 4):
        weight = sub / 3.0
        cycle_value = upsample((1.0 - weight) * old_tiles + weight * new_tiles)
        fine_ez, fine_hx, fine_hy = fine_substep(fine_ez, fine_hx, fine_hy, damp, gain, inbox, middle, border, cycle_value)
    return fine_ez, fine_hx, fine_hy


def reference(coarse_ez, coarse_hx, coarse_hy, coarse_ids, mat_eps, mat_sig, fine_ez, fine_hx, fine_hy, fine_ids, boxes, src_cells, src_wave, rcv_cells):
    blocks_x = boxes.shape[0]
    blocks_y = boxes.shape[1]
    rows, cols = coarse_ez.shape
    block_rows = rows // blocks_x
    block_cols = cols // blocks_y
    damp, gain = coefficients(coarse_ids, mat_eps, mat_sig, 1.0)
    fine_damp, fine_gain = coefficients(fine_ids, mat_eps, mat_sig, 3.0)
    inbox, middle = flat_masks(boxes)
    border = inbox & jnp.logical_not(middle)
    coarse_mid = from_tiles(box_masks(boxes, TILE, 1)[1], block_rows, block_cols)
    ez, hx, hy = coarse_ez, coarse_hx, coarse_hy
    samples = []
    for step in range(STEPS):
        ez_next_col = jnp.pad(ez[:, 1:], ((0, 0), (0, 1)))
        ez_next_row = jnp.pad(ez[1:, :], ((0, 1), (0, 0)))
        hx = hx - HCOEF * (ez_next_col - ez)
        hy = hy + HCOEF * (ez_next_row - ez)
        hy_prev = jnp.pad(hy[:-1, :], ((1, 0), (0, 0)))
        hx_prev = jnp.pad(hx[:, :-1], ((0, 0), (1, 0)))
        curl = (hy - hy_prev) - (hx - hx_prev)
        drive = jnp.zeros((rows * cols,), jnp.float32).at[src_cells].add(src_wave[step]).reshape(rows, cols)
        new = damp * ez + gain * curl + drive
        old_tiles = to_tiles(ez, blocks_x, blocks_y)
        new_tiles = to_tiles(new, blocks_x, blocks_y)
        fine_ez, fine_hx, fine_hy = fine_round(fine_ez, fine_hx, fine_hy, fine_damp, fine_gain, inbox, middle, border, old_tiles, new_tiles)
        back = from_tiles(cell_means(fine_ez), block_rows, block_cols)
        ez = jnp.where(coarse_mid, back, new)
        samples.append(ez.reshape(-1)[rcv_cells])
    return ez, hx, hy, fine_ez, fine_hx, fine_hy, jnp.stack(samples)
```

```python
import functools

import jax
import jax.numpy as jnp
from jax import lax
from jax.experimental import pallas as pl
from jax.experimental.pallas import tpu as pltpu
from jax.sharding import PartitionSpec as P

MESH = pl.DeviceIdType.MESH
NA = 32
NB = 8
STEPS = 3
f32 = jnp.float32
i32 = jnp.int32


def lanes():
    return lax.broadcasted_iota(i32, (8, 128), 1)


def sublanes():
    return lax.broadcasted_iota(i32, (8, 128), 0)


def swap_blocks(x, sub, lg):
    for k in range(3):
        bs = (sub >> k) & 1
        bl = (lg >> k) & 1
        step = 16 << k
        down = pltpu.roll(pltpu.roll(x, 1 << k, 0), 128 - step, 1)
        up = pltpu.roll(pltpu.roll(x, 8 - (1 << k), 0), step, 1)
        x = jnp.where(bs == bl, x, jnp.where(bs == 1, down, up))
    return x


def lane_gather(x, idx):
    return jnp.take_along_axis(x, idx, axis=1)


def div3(x):
    return (x * 21846) >> 16


def div48(x):
    return div3(x >> 4)


def step_tables(eps, sig, ratio):
    loss = sig / (eps * ratio)
    return (1.0 - loss) / (1.0 + loss), 0.5 / (eps * (1.0 + loss))


def kernel(
    ez_in, hx_in, hy_in, ids_in, eps_in, sig_in, fez_in, fhx_in, fhy_in, fids_in, box_in, src_in, wave_in, rcv_in,
    ez_out, hx_out, hy_out, fez_out, fhx_out, fhy_out, tr_out,
    HE, IDS, PB, PEL, PER, E2, S1, R1, S2, R2, O1, RO1, O2, RO2, TS, TB, TS2, TG,
    FE, FX, FY, FI, FD, FG, CH, U, DB, BM, IDX, TAB, NEWC, MC,
    in_sem, halo_sem, halo_send, send_sem, recv_sem, out_sem,
):
    grp = lax.axis_index("grp")
    a = lax.axis_index("gx")
    gy = lax.axis_index("gy")
    b = grp * 4 + gy

    def dev(na, nb):
        return (nb // 4, na, nb % 4)

    am, ap = lax.rem(a + NA - 1, NA), lax.rem(a + 1, NA)
    bm, bp = lax.rem(b + NB - 1, NB), lax.rem(b + 1, NB)

    barrier = pltpu.get_barrier_semaphore()

    def signal(na, nb):
        pl.semaphore_signal(barrier, inc=1, device_id=dev(na, nb), device_id_type=MESH)

    for na in (am, ap):
        for nb in (bm, bp):
            signal(na, nb)
    for d in range(1, NB):
        signal(a, lax.rem(b + d, NB))

    def signal_gx(d, carry):
        signal(lax.rem(a + d, NA), b)
        return carry

    lax.fori_loop(1, NA, signal_gx, 0)

    loads = []
    for j, (src, dst) in enumerate((
        (ez_in, HE.at[0, pl.ds(8, 64), :]),
        (hx_in, HE.at[1, pl.ds(8, 64), :]),
        (hy_in, HE.at[2, pl.ds(8, 64), :]),
        (ids_in, IDS),
        (fids_in, FI),
        (fez_in, FE),
        (fhx_in, FX),
        (fhy_in, FY),
    )):
        copy = pltpu.make_async_copy(src, dst, in_sem.at[j])
        copy.start()
        loads.append(copy)

    lane = lanes()
    sub = sublanes()
    lg = lane >> 4

    TAB[pl.ds(0, 8), :] = jnp.ones((8, 128), f32)
    TAB[pl.ds(8, 8), :] = jnp.zeros((8, 128), f32)
    TAB[pl.ds(0, 8), pl.ds(0, 8)] = jnp.broadcast_to(eps_in[...], (8, 8))
    TAB[pl.ds(8, 8), pl.ds(0, 8)] = jnp.broadcast_to(sig_in[...], (8, 8))
    eps, sig = TAB[pl.ds(0, 8), :], TAB[pl.ds(8, 8), :]
    damp1, gain1 = step_tables(eps, sig, 1.0)
    damp3, gain3 = step_tables(eps, sig, 3.0)

    for g in range(9):
        pos = lane + 128 * g
        p = div48(pos)
        q = pos - 48 * p
        IDX[pl.ds(8 * g, 8), :] = div3(p) * 16 + div3(q)

    for copy in loads[:4]:
        copy.wait()
    HE[3, pl.ds(8, 64), :] = IDS[...].astype(f32)

    def pack1(v, carry):
        ci, h = v // 2, lax.rem(v, 2)
        for k in range(4):
            x = HE[k, pl.ds(pl.multiple_of(8 + 8 * v, 8), 8), :]
            S1[pl.ds(ci * 128 + 2 * k + h, 8, stride=16), :] = swap_blocks(x, sub, lg)
        return carry

    lax.fori_loop(0, 8, pack1, 0)
    row32 = lax.broadcasted_iota(i32, (32, 32), 0)
    col32 = lax.broadcasted_iota(i32, (32, 32), 1)
    lane32 = lax.broadcasted_iota(i32, (32, 128), 1)
    box_rows = jnp.zeros((32, 128), f32)
    for k in range(4):
        one = jnp.broadcast_to(box_in[pl.ds(k, 1), :], (32, 32)).astype(f32)
        value = jnp.sum(jnp.where(row32 == col32, one, 0.0), axis=1, keepdims=True)
        box_rows = jnp.where(lane32 == k, value, box_rows)
    S1[pl.ds(8, 32, stride=16), :] = box_rows

    lane64 = lax.broadcasted_iota(i32, (64, 128), 1)
    packed = jnp.zeros((64, 128), f32)
    for k in range(4):
        near = (lane64 - 8 * k) & 127
        x = HE[k, pl.ds(8, 64), :]
        packed = jnp.where((near < 3) | (near >= 125), pltpu.roll(x, 8 * k, 1) if k else x, packed)
    PB[...] = packed

    pl.semaphore_wait(barrier, (NA - 1) + (NB - 1) + 4)

    halos = []

    def halo(j, src, dst, na, nb):
        copy = pltpu.make_async_remote_copy(
            src_ref=src, dst_ref=dst, send_sem=halo_send.at[j], recv_sem=halo_sem.at[j],
            device_id=dev(na, nb), device_id_type=MESH,
        )
        copy.start()
        halos.append(copy)

    halo(0, HE.at[:, pl.ds(64, 8), :], HE.at[:, pl.ds(0, 8), :], ap, b)
    halo(1, HE.at[:, pl.ds(8, 8), :], HE.at[:, pl.ds(72, 8), :], am, b)
    halo(2, PB, PEL.at[pl.ds(8, 64), :], a, bp)
    halo(3, PB, PER.at[pl.ds(8, 64), :], a, bm)
    halo(4, PB.at[pl.ds(56, 8), :], PEL.at[pl.ds(0, 8), :], ap, bp)
    halo(5, PB.at[pl.ds(56, 8), :], PER.at[pl.ds(0, 8), :], ap, bm)
    halo(6, PB.at[pl.ds(0, 8), :], PEL.at[pl.ds(72, 8), :], am, bp)
    halo(7, PB.at[pl.ds(0, 8), :], PER.at[pl.ds(72, 8), :], am, bm)

    def gx_copy(j, src, dst, slot, rows, n, mine):
        return pltpu.make_async_remote_copy(
            src_ref=src.at[pl.ds(pl.multiple_of(n * slot, slot), rows), :],
            dst_ref=dst.at[pl.ds(pl.multiple_of(mine * slot, slot), rows), :],
            send_sem=send_sem.at[j], recv_sem=recv_sem.at[j],
            device_id=dev(n, b), device_id_type=MESH,
        )

    def exchange(j, src, dst, slot, rows, same=False):
        def body(d, carry):
            n = lax.rem(a + d, NA)
            pltpu.make_async_remote_copy(
                src_ref=src.at[pl.ds(0 if same else pl.multiple_of(n * slot, slot), rows), :],
                dst_ref=dst.at[pl.ds(pl.multiple_of(a * slot, slot), rows), :],
                send_sem=send_sem.at[j], recv_sem=recv_sem.at[j],
                device_id=dev(n, b), device_id_type=MESH,
            ).start()
            return carry

        lax.fori_loop(1, NA, body, 0)
        own = pl.multiple_of(a * slot, slot)
        dst[pl.ds(own, rows), :] = src[pl.ds(0 if same else own, rows), :]

    def received(j, buf, rows):
        total = (NA - 1) * rows
        return pltpu.make_async_copy(buf.at[pl.ds(0, total), :], buf.at[pl.ds(0, total), :], recv_sem.at[j])

    def sent(j, buf, rows):
        total = (NA - 1) * rows
        return pltpu.make_async_copy(buf.at[pl.ds(0, total), :], buf.at[pl.ds(0, total), :], send_sem.at[j])

    exchange(0, S1, R1, 16, 9)

    loads[4].wait()

    def fine_coef(v, carry):
        rows = pl.ds(pl.multiple_of(8 * v, 8), 8)
        ids = FI[rows, :]
        FD[rows, :] = lane_gather(damp3, ids)
        FG[rows, :] = lane_gather(gain3, ids)
        return carry

    lax.fori_loop(0, 72, fine_coef, 0)

    for copy in halos:
        copy.wait()
    lane80 = lax.broadcasted_iota(i32, (80, 128), 1)
    row80 = lax.broadcasted_iota(i32, (80, 128), 0)
    row_g = row80 + (a * 64 - 8)
    col_m = lane80 + b * 128
    col_s = jnp.where(lane80 < 64, col_m + 128, col_m - 128)
    row_ok = (row_g >= 0) & (row_g < NA * 64)
    ok_m = jnp.where(row_ok, 1.0, 0.0)
    ok_s = jnp.where(row_ok & (col_s >= 0) & (col_s < NB * 128), 1.0, 0.0)

    def sides(k):
        left, right = PEL[...], PER[...]
        if k:
            left, right = pltpu.roll(left, 128 - 8 * k, 1), pltpu.roll(right, 128 - 8 * k, 1)
        return jnp.where(lane80 >= 125, left, jnp.where(lane80 < 3, right, 0.0))

    pair_ez, pair_hx, pair_hy = ((HE[k] * ok_m, sides(k) * ok_s) for k in range(3))

    def coef80(table, ids, ok):
        parts = [lane_gather(table, ids[8 * r : 8 * r + 8, :].astype(i32)) for r in range(10)]
        return jnp.concatenate(parts, axis=0) * ok

    ids_m, ids_s = HE[3], sides(3)
    pair_damp = (coef80(damp1, ids_m, ok_m), coef80(damp1, ids_s, ok_s))
    pair_gain = (coef80(gain1, ids_m, ok_m), coef80(gain1, ids_s, ok_s))

    def right_of(x):
        m, s = pltpu.roll(x[0], 127, 1), pltpu.roll(x[1], 127, 1)
        return jnp.where(lane80 < 127, m, s), jnp.where(lane80 < 127, s, m)

    def left_of(x):
        m, s = pltpu.roll(x[0], 1, 1), pltpu.roll(x[1], 1, 1)
        return jnp.where(lane80 >= 1, m, s), jnp.where(lane80 >= 1, s, m)

    def below(x):
        return pltpu.roll(x[0], 79, 0), pltpu.roll(x[1], 79, 0)

    def above(x):
        return pltpu.roll(x[0], 1, 0), pltpu.roll(x[1], 1, 0)

    def both(fn, *pairs):
        return tuple(fn(*(p[i] for p in pairs)) for i in range(2))

    src_i = [src_in[0, k] >> 10 for k in range(4)]
    src_j = [src_in[0, k] & 1023 for k in range(4)]

    def h_step(ez, hx, hy):
        hx = both(lambda h, e, r, k: (h - 0.5 * (r - e)) * k, hx, ez, right_of(ez), (ok_m, ok_s))
        hy = both(lambda h, e, r, k: (h + 0.5 * (r - e)) * k, hy, ez, below(ez), (ok_m, ok_s))
        return hx, hy

    for n in range(2):
        pair_hx, pair_hy = h_step(pair_ez, pair_hx, pair_hy)
        drive = []
        for col in (col_m, col_s):
            total = jnp.zeros((80, 128), f32)
            for k in range(4):
                total = total + jnp.where((row_g == src_i[k]) & (col == src_j[k]), wave_in[n, k], 0.0)
            drive.append(total)
        pair_ez = both(
            lambda d, e, g, hy, hu, hx, hl, s: d * e + g * ((hy - hu) - (hx - hl)) + s,
            pair_damp, pair_ez, pair_gain, pair_hy, above(pair_hy), pair_hx, left_of(pair_hx), tuple(drive),
        )
        E2[n] = pair_ez[0][8:72, :]
    pair_hx, pair_hy = h_step(pair_ez, pair_hx, pair_hy)
    E2[2] = jnp.where((row80 & 15) == 8, above(pair_hy)[0], pair_hy[0])[8:72, :]
    E2[3] = jnp.where((lane80 & 15) == 0, left_of(pair_hx)[0], pair_hx[0])[8:72, :]

    e4, t16 = (lane >> 4) & 3, lane & 15
    frame_idx = jnp.where(
        e4 == 0, t16,
        jnp.where(e4 == 1, 112 + t16, jnp.where(e4 == 2, 16 * (t16 & 7), 16 * (t16 & 7) + 15)),
    )
    from_h1 = jnp.where(e4 == 0, 0, jnp.where(e4 == 1, 1, t16 >> 3)) == 1

    def pack2(ci, carry):
        got = []
        for k in range(4):
            halves = []
            for h in range(2):
                x = E2[k, pl.ds(pl.multiple_of(16 * ci + 8 * h, 8), 8), :]
                halves.append(lane_gather(swap_blocks(x, sub, lg), frame_idx))
            got.append(jnp.where(from_h1, halves[1], halves[0]))
        S2[pl.ds(ci * 64, 8, stride=8), :] = jnp.where(lane < 64, got[0], got[1])
        S2[pl.ds(ci * 64 + 1, 8, stride=8), :] = jnp.where((lane & 63) < 32, got[2], got[3])
        return carry

    lax.fori_loop(0, 4, pack2, 0)
    exchange(1, S2, R2, 8, 2)

    received(0, R1, 9).wait()
    for copy in loads[5:]:
        copy.wait()

    def from1(k):
        return tuple(R1[pl.ds(2 * k + h, 32, stride=16), :] for h in range(2))

    ez, hx, hy, ids_c = (from1(k) for k in range(4))

    def coef32(table, ids):
        parts = [lane_gather(table, ids[8 * r : 8 * r + 8, :].astype(i32)) for r in range(4)]
        return jnp.concatenate(parts, axis=0)

    damp = tuple(coef32(damp1, x) for x in ids_c)
    gain = tuple(coef32(gain1, x) for x in ids_c)
    NEWC[pl.ds(0, 32), :], NEWC[pl.ds(32, 32), :] = ez

    def prepare(tg, carry):
        base = tg * 144
        box = R1[pl.ds(tg * 128 + 8, 8, stride=16), :]
        lo_i, lo_j, n_i, n_j = (jnp.broadcast_to(box[:, k : k + 1], (8, 128)).astype(i32) for k in range(4))
        hi_i, hi_j = lo_i + n_i, lo_j + n_j
        old = [NEWC[pl.ds(pl.multiple_of(32 * h + 8 * tg, 8), 8), :] for h in range(2)]
        for g in range(18):
            rows = pl.ds(base + g, 8, stride=18)
            idx = IDX[pl.ds(8 * (g % 9), 8), :]
            ci = (idx >> 4) + (8 if g >= 9 else 0)
            cj = idx & 15
            inbox = (ci >= lo_i) & (ci < hi_i) & (cj >= lo_j) & (cj < hi_j)
            middle = (ci > lo_i) & (ci < hi_i - 1) & (cj > lo_j) & (cj < hi_j - 1)
            fin = jnp.where(inbox, 1.0, 0.0)
            fmid = jnp.where(middle, 1.0, 0.0)
            fbor = fin - fmid
            FX[rows, :] = FX[rows, :] * fin
            FY[rows, :] = FY[rows, :] * fin
            CH[rows, :] = 0.5 * fin
            FD[rows, :] = FD[rows, :] * fmid
            FG[rows, :] = FG[rows, :] * fmid
            BM[rows, :] = fbor
            U[rows, :] = fbor * lane_gather(old[g // 9], idx)
        return carry

    lax.fori_loop(0, 4, prepare, 0)

    mean_pos = 144 * (lane >> 4) + 3 * (lane & 15)
    mean_idx = mean_pos & 127
    mean_group = mean_pos >> 7

    def fine_round(tg, carry):
        base = tg * 144

        def at(g):
            return pl.ds(base + g, 8, stride=18)

        new = [NEWC[pl.ds(pl.multiple_of(32 * h + 8 * tg, 8), 8), :] for h in range(2)]
        for g in range(18):
            value = BM[at(g), :] * lane_gather(new[g // 9], IDX[pl.ds(8 * (g % 9), 8), :])
            DB[at(g), :] = value - U[at(g), :]
            U[at(g), :] = value

        def substep(m, carry):
            behind = (2 - m).astype(f32) * (1.0 / 3.0)
            e = FE[at(0), :]
            e1, e48 = pltpu.roll(e, 127, 1), pltpu.roll(e, 80, 1)
            x1 = y48 = None
            for g in range(18):
                if g < 17:
                    e_next = FE[at(g + 1), :]
                    n1, n48 = pltpu.roll(e_next, 127, 1), pltpu.roll(e_next, 80, 1)
                c = CH[at(g), :]
                hx_g = FX[at(g), :] - c * (jnp.where(lane < 127, e1, n1) - e)
                hy_g = FY[at(g), :] + c * (jnp.where(lane < 80, e48, n48) - e)
                FX[at(g), :] = hx_g
                FY[at(g), :] = hy_g
                rx, ry = pltpu.roll(hx_g, 1, 1), pltpu.roll(hy_g, 48, 1)
                if g == 0:
                    x1, y48 = rx, ry
                curl = (hy_g - jnp.where(lane >= 48, ry, y48)) - (hx_g - jnp.where(lane >= 1, rx, x1))
                FE[at(g), :] = FD[at(g), :] * e + FG[at(g), :] * curl + (U[at(g), :] - behind * DB[at(g), :])
                x1, y48 = rx, ry
                e, e1, e48 = e_next, n1, n48
            return carry

        lax.fori_loop(0, 3, substep, 0)

        def sums(g):
            x = FE[at(g), :]
            return x, pltpu.roll(x, 127, 1), pltpu.roll(x, 126, 1)

        for h in range(2):
            groups = [sums(9 * h + g) for g in range(9)]
            groups.append(sums(9) if h == 0 else groups[8])
            rowsum = [
                groups[g][0]
                + jnp.where(lane < 127, groups[g][1], groups[min(g + 1, 9)][1])
                + jnp.where(lane < 126, groups[g][2], groups[min(g + 1, 9)][2])
                for g in range(10)
            ]
            r48 = [pltpu.roll(x, 80, 1) for x in rowsum]
            r96 = [pltpu.roll(x, 32, 1) for x in rowsum]
            total = jnp.zeros((8, 128), f32)
            for g in range(9):
                s = rowsum[g] + jnp.where(lane < 80, r48[g], r48[g + 1]) + jnp.where(lane < 32, r96[g], r96[g + 1])
                total = jnp.where(mean_group == g, lane_gather(s, mean_idx), total)
            MC[pl.ds(pl.multiple_of(32 * h + 8 * tg, 8), 8), :] = total * (1.0 / 9.0)
        return carry

    row_in = lane32 >> 4
    col_in = lane32 & 15
    boxes = R1[pl.ds(8, 32, stride=16), :]
    lo_i, lo_j, n_i, n_j = (jnp.broadcast_to(boxes[:, k : k + 1], (32, 128)).astype(i32) for k in range(4))
    mid = tuple(
        (row_in + 8 * h > lo_i) & (row_in + 8 * h < lo_i + n_i - 1) & (col_in > lo_j) & (col_in < lo_j + n_j - 1)
        for h in range(2)
    )
    edge_col = (col_in == 0) | (col_in == 15)
    frame = (edge_col | (row_in == 0), edge_col | (row_in == 7))
    tile32 = lax.broadcasted_iota(i32, (32, 128), 0)
    my_ci, my_cj = a // 8, lax.rem(a, 8)
    src_tile, src_cell = [], []
    for k in range(4):
        i, j = src_i[k], src_j[k]
        here = ((i & 63) >> 4 == my_ci) & ((j & 127) >> 4 == my_cj) & (j >> 7 == b)
        src_tile.append(jnp.where(here, i >> 6, -1))
        src_cell.append((i & 15) * 16 + (j & 15))
    rcv = jnp.broadcast_to(rcv_in[...], (8, 128))
    ri, rj = rcv >> 10, rcv & 1023
    r_here = (((ri & 63) >> 4) == my_ci) & (((rj & 127) >> 4) == my_cj) & ((rj >> 7) == b)
    r_tile = jnp.where(r_here, ri >> 6, -1)
    r_cell = (ri & 15) * 16 + (rj & 15)
    r_idx, r_half = r_cell & 127, r_cell >> 7

    def c_right(x):
        return tuple(pltpu.roll(v, 127, 1) for v in x)

    def c_left(x):
        return tuple(pltpu.roll(v, 1, 1) for v in x)

    def c_below(x):
        y = tuple(pltpu.roll(v, 112, 1) for v in x)
        return jnp.where(lane32 < 112, y[0], y[1]), y[1]

    def c_above(x):
        y = tuple(pltpu.roll(v, 16, 1) for v in x)
        return y[0], jnp.where(lane32 >= 16, y[1], y[0])

    framed = None
    for n in range(STEPS):
        hx = both(lambda h, e, r: h - 0.5 * (r - e), hx, ez, c_right(ez))
        hy = both(lambda h, e, r: h + 0.5 * (r - e), hy, ez, c_below(ez))
        hx_left, hy_up = c_left(hx), c_above(hy)
        if n == 2:
            edge = R2[pl.ds(1, 32, stride=8), :]

            def spread(idx):
                parts = [lane_gather(edge[8 * r : 8 * r + 8, :], idx) for r in range(4)]
                return jnp.concatenate(parts, axis=0)

            w1 = tuple(spread(t16 + 16 * h) for h in range(2))
            w2 = tuple(spread(jnp.where(t16 == 15, 48, 32) + (lane >> 4) + 8 * h) for h in range(2))
            hy = (hy[0], jnp.where(row_in == 7, w1[1], hy[1]))
            hx = tuple(jnp.where(col_in == 15, w2[h], hx[h]) for h in range(2))
            hy_up = (jnp.where(row_in == 0, w1[0], hy_up[0]), hy_up[1])
            hx_left = tuple(jnp.where(col_in == 0, w2[h], hx_left[h]) for h in range(2))
            for h in range(2):
                O1[pl.ds(h, 32, stride=8), :] = hx[h]
                O1[pl.ds(2 + h, 32, stride=8), :] = hy[h]
            exchange(2, O1, RO1, 8, 4)
        drive = []
        for h in range(2):
            total = jnp.zeros((32, 128), f32)
            for k in range(4):
                total = total + jnp.where(
                    (tile32 == src_tile[k]) & (lane32 + 128 * h == src_cell[k]), wave_in[n, k], 0.0
                )
            drive.append(total)
        new = both(
            lambda d, e, g, y, yu, x, xl, s: d * e + g * ((y - yu) - (x - xl)) + s,
            damp, ez, gain, hy, hy_up, hx, hx_left, tuple(drive),
        )
        NEWC[pl.ds(0, 32), :], NEWC[pl.ds(32, 32), :] = new
        lax.fori_loop(0, 4, fine_round, 0)
        if n == 0:
            received(1, R2, 2).wait()
        if n < 2:
            rim = R2[pl.ds(0, 32, stride=8), :]
            out = []
            for h in range(2):
                r = (lane >> 4) + 8 * h
                slot = jnp.where(
                    r == 0, t16, jnp.where(r == 15, 16 + t16, jnp.where(t16 == 0, 32 + r, 48 + r))
                )
                slot = (slot & 63) + 64 * n
                parts = [lane_gather(rim[8 * q : 8 * q + 8, :], slot) for q in range(4)]
                out.append(jnp.where(frame[h], jnp.concatenate(parts, axis=0), new[h]))
            new = tuple(out)
        ez = both(lambda m, x, y: jnp.where(m, x, y), mid, (MC[pl.ds(0, 32), :], MC[pl.ds(32, 32), :]), new)
        if n == 2:
            for h in range(2):
                O2[pl.ds(h, 32, stride=8), :] = ez[h]
            exchange(3, O2, RO2, 8, 2)
        picked = jnp.zeros((8, 128), f32)
        for h in range(2):
            for q in range(4):
                got = lane_gather(ez[h][8 * q : 8 * q + 8, :], r_idx)
                picked = picked + jnp.where((r_tile == sub + 8 * q) & (r_half == h), got, 0.0)
        TS[pl.ds(n, 1), :] = jnp.sum(picked, axis=0, keepdims=True)

    for d in range(1, NB):
        n = lax.rem(b + d, NB)
        pltpu.make_async_remote_copy(
            src_ref=TS.at[pl.ds(0, 3), :],
            dst_ref=TB.at[pl.ds(pl.multiple_of(8 * b, 8), 3), :],
            send_sem=send_sem.at[4], recv_sem=recv_sem.at[4],
            device_id=dev(a, n), device_id_type=MESH,
        ).start()
    TB[pl.ds(pl.multiple_of(8 * b, 8), 3), :] = TS[pl.ds(0, 3), :]

    stores = []
    for j, (src, dst) in enumerate(((FE, fez_out), (FX, fhx_out), (FY, fhy_out))):
        copy = pltpu.make_async_copy(src, dst, out_sem.at[j])
        copy.start()
        stores.append(copy)

    seven = (NB - 1) * 3
    pltpu.make_async_copy(TB.at[pl.ds(0, seven), :], TB.at[pl.ds(0, seven), :], recv_sem.at[4]).wait()
    for n in range(STEPS):
        TS2[pl.ds(n, 1), :] = jnp.sum(TB[pl.ds(n, 8, stride=8), :], axis=0, keepdims=True)
    exchange(5, TS2, TG, 8, 3, same=True)

    received(2, RO1, 4).wait()

    def unpack(src, first, dst):
        def body(ci, carry):
            for h in range(2):
                x = src[pl.ds(ci * 64 + first + h, 8, stride=8), :]
                dst[pl.ds(pl.multiple_of(16 * ci + 8 * h, 8), 8), :] = swap_blocks(x, sub, lg)
            return carry

        lax.fori_loop(0, 4, body, 0)

    unpack(RO1, 0, hx_out)
    unpack(RO1, 2, hy_out)
    received(3, RO2, 2).wait()
    unpack(RO2, 0, ez_out)
    received(5, TG, 3).wait()
    for n in range(STEPS):
        tr_out[pl.ds(n, 1), :] = jnp.sum(TG[pl.ds(n, 32, stride=8), :], axis=0, keepdims=True)

    for copy in stores:
        copy.wait()
    for j, buf, rows in ((0, S1, 9), (1, S2, 2), (2, O1, 4), (3, O2, 2), (5, TG, 3)):
        sent(j, buf, rows).wait()
    pltpu.make_async_copy(TB.at[pl.ds(0, seven), :], TB.at[pl.ds(0, seven), :], send_sem.at[4]).wait()


def shards(
    coarse_ez, coarse_hx, coarse_hy, coarse_ids, mat_eps, mat_sig,
    fine_ez, fine_hx, fine_hy, fine_ids, boxes, src_cells, src_wave, rcv_cells,
):
    fine_shape = fine_ez.shape
    flat = (576, 128)
    anywhere = pl.BlockSpec(memory_space=pl.ANY)
    vmem = pl.BlockSpec(memory_space=pltpu.VMEM)
    smem = pl.BlockSpec(memory_space=pltpu.SMEM)
    block = jax.ShapeDtypeStruct((64, 128), f32)
    fine = jax.ShapeDtypeStruct(flat, f32)

    def v(*shape, dtype=f32):
        return pltpu.VMEM(shape, dtype)

    outs = pl.pallas_call(
        kernel,
        name="nested",
        out_shape=(block, block, block, fine, fine, fine, jax.ShapeDtypeStruct((3, 128), f32)),
        in_specs=[anywhere] * 4 + [vmem] * 2 + [anywhere] * 4 + [vmem, smem, smem, vmem],
        out_specs=(vmem, vmem, vmem, anywhere, anywhere, anywhere, vmem),
        scratch_shapes=[
            v(4, 80, 128), v(64, 128, dtype=i32), v(64, 128), v(80, 128), v(80, 128), v(4, 64, 128),
            v(512, 128), v(512, 128), v(256, 128), v(256, 128),
            v(256, 128), v(256, 128), v(256, 128), v(256, 128),
            v(8, 128), v(64, 128), v(8, 128), v(256, 128),
            v(576, 128), v(576, 128), v(576, 128), v(576, 128, dtype=i32),
            v(576, 128), v(576, 128), v(576, 128), v(576, 128), v(576, 128), v(576, 128),
            v(72, 128, dtype=i32), v(16, 128), v(64, 128), v(64, 128),
            pltpu.SemaphoreType.DMA((8,)), pltpu.SemaphoreType.DMA((8,)), pltpu.SemaphoreType.DMA((8,)),
            pltpu.SemaphoreType.DMA((6,)), pltpu.SemaphoreType.DMA((6,)), pltpu.SemaphoreType.DMA((3,)),
        ],
        compiler_params=pltpu.CompilerParams(collective_id=0, has_side_effects=True),
    )(
        coarse_ez, coarse_hx, coarse_hy, coarse_ids,
        mat_eps.reshape(1, 8), mat_sig.reshape(1, 8),
        fine_ez.reshape(flat), fine_hx.reshape(flat), fine_hy.reshape(flat), fine_ids.reshape(flat),
        boxes.reshape(32, 4).T, src_cells.reshape(1, 4), src_wave, rcv_cells.reshape(1, 128),
    )
    return outs[:3] + tuple(x.reshape(fine_shape) for x in outs[3:6]) + (outs[6],)


def solution(mesh):
    coarse = P("gx", ("grp", "gy"))
    tiles = P(None, ("grp", "gy"), "gx", None)
    in_specs = (
        coarse, coarse, coarse, coarse, P(), P(), tiles, tiles, tiles, tiles,
        P("gx", ("grp", "gy"), None, None), P(), P(), P(),
    )
    out_specs = (coarse, coarse, coarse, tiles, tiles, tiles, P())
    return jax.shard_map(shards, mesh=mesh, in_specs=in_specs, out_specs=out_specs, check_vma=False)
```

```python
import functools

import jax
import jax.numpy as jnp
from jax import lax
from jax.experimental import pallas as pl
from jax.experimental.pallas import tpu as pltpu
from jax.sharding import PartitionSpec as P

MESH = pl.DeviceIdType.MESH
NA = 32
NB = 8
STEPS = 3
f32 = jnp.float32
i32 = jnp.int32


def lanes():
    return lax.broadcasted_iota(i32, (8, 128), 1)


def sublanes():
    return lax.broadcasted_iota(i32, (8, 128), 0)


def swap_blocks(x, sub, lg):
    for k in range(3):
        bs = (sub >> k) & 1
        bl = (lg >> k) & 1
        step = 16 << k
        down = pltpu.roll(pltpu.roll(x, 1 << k, 0), 128 - step, 1)
        up = pltpu.roll(pltpu.roll(x, 8 - (1 << k), 0), step, 1)
        x = jnp.where(bs == bl, x, jnp.where(bs == 1, down, up))
    return x


def lane_gather(x, idx):
    return jnp.take_along_axis(x, idx, axis=1)


def div(x, n):
    return (x * ((1 << 20) // n + 1)) >> 20


FINE = 48


def sources_of_cells():
    need = [set() for _ in range(18)]
    back = [set() for _ in range(18)]
    for p in range(FINE):
        for q in range(FINE):
            u, g = 3 * (p % 6) + q % 3, (p * FINE + q) // 128
            need[u].add(g)
            back[g].add(u)
    return [sorted(x) for x in need], [sorted(x) for x in back]


NEED, BACK = sources_of_cells()


def pick(table, ids):
    bits = [(ids & (1 << k)) != 0 for k in range(3)]
    for bit in bits:
        table = [jnp.where(bit, table[i + 1], table[i]) for i in range(0, len(table), 2)]
    return table[0]


def step_tables(eps, sig, ratio):
    loss = sig / (eps * ratio)
    return (1.0 - loss) / (1.0 + loss), 0.5 / (eps * (1.0 + loss))


def kernel(
    ez_in, hx_in, hy_in, ids_in, eps_in, sig_in, fez_in, fhx_in, fhy_in, fids_in, box_in, src_in, wave_in, rcv_in,
    ez_out, hx_out, hy_out, fez_out, fhx_out, fhy_out, tr_out,
    HE, IDS, PB, PEL, PER, E2, S1, R1, S2, R2, O1, RO1, O2, RO2, TS, TB, TS2, TG,
    FI, FD, FG, WE, WX, WY, IDX, SEL, TAB, CO, BOX, SRC, WAVE, RCV, EPS, SIG,
    in_sem, halo_sem, halo_send, send_sem, recv_sem, stage_sem,
):
    FE, FX, FY = fez_out, fhx_out, fhy_out
    grp = lax.axis_index("grp")
    a = lax.axis_index("gx")
    gy = lax.axis_index("gy")
    b = grp * 4 + gy

    def dev(na, nb):
        return (nb // 4, na, nb % 4)

    am, ap = lax.rem(a + NA - 1, NA), lax.rem(a + 1, NA)
    bm, bp = lax.rem(b + NB - 1, NB), lax.rem(b + 1, NB)

    loads = []
    for j, (source, dst) in enumerate((
        (ez_in, HE.at[0, pl.ds(8, 64), :]),
        (hx_in, HE.at[1, pl.ds(8, 64), :]),
        (hy_in, HE.at[2, pl.ds(8, 64), :]),
        (ids_in, IDS),
        (fids_in, FI),
        (fez_in, FE),
        (fhx_in, FX),
        (fhy_in, FY),
        (box_in, BOX),
        (eps_in, EPS),
        (sig_in, SIG),
        (rcv_in, RCV),
        (src_in, SRC),
        (wave_in, WAVE),
    )):
        copy = pltpu.make_async_copy(source, dst, in_sem.at[j])
        copy.start()
        loads.append(copy)

    barrier = pltpu.get_barrier_semaphore()

    def signal(na, nb):
        pl.semaphore_signal(barrier, inc=1, device_id=dev(na, nb), device_id_type=MESH)

    y, z = a // 8, lax.rem(a, 8)
    for na in (am, ap):
        for nb in (bm, b, bp):
            signal(na, nb)
    for d in range(1, NB):
        signal(a, lax.rem(b + d, NB))
    for d in range(1, 8):
        signal(y * 8 + lax.rem(z + d, 8), b)
    y_peers = [lax.rem(y + d, 4) * 8 + z for d in range(1, 4)]
    for n in y_peers:
        signal(n, b)

    lane = lanes()
    sub = sublanes()
    lg = lane >> 4

    for g in range(18):
        pos = lane + 128 * g
        p = div(pos, 48)
        q = pos - 48 * p
        pb, j = div(p, 6), div(q, 3)
        IDX[pl.ds(8 * g, 8), :] = 16 * pb + j
        SEL[pl.ds(8 * g, 8), :] = 3 * (p - 6 * pb) + (q - 3 * j)
    cell_pos = 288 * (lane >> 4) + 3 * (lane & 15)

    def flat_rows(tg, g):
        return pl.ds(tg * 144 + g, 8, stride=18)

    def cell_rows(tg, u):
        return pl.ds(pl.multiple_of(tg * 144 + 8 * u, 8), 8)

    def to_cells(src, put):
        def body(tg, carry):
            flat = [src[flat_rows(tg, g), :] for g in range(18)]
            for u in range(18):
                pos = cell_pos + (48 * (u // 3) + u % 3)
                idx, group = pos & 127, pos >> 7
                value = lane_gather(flat[NEED[u][0]], idx)
                for g in NEED[u][1:]:
                    value = jnp.where(group == g, lane_gather(flat[g], idx), value)
                put(tg, u, value)
            return carry

        lax.fori_loop(0, 4, body, 0)

    def put_in(dst):
        def put(tg, u, value):
            dst[cell_rows(tg, u), :] = value

        return put

    def from_cells(src, dst):
        def body(tg, carry):
            cells = [src[cell_rows(tg, u), :] for u in range(18)]
            for g in range(18):
                idx, group = IDX[pl.ds(8 * g, 8), :], SEL[pl.ds(8 * g, 8), :]
                value = lane_gather(cells[BACK[g][0]], idx)
                for u in BACK[g][1:]:
                    value = jnp.where(group == u, lane_gather(cells[u], idx), value)
                dst[flat_rows(tg, g), :] = value
            return carry

        lax.fori_loop(0, 4, body, 0)

    for copy in loads[:4] + loads[8:]:
        copy.wait()
    HE[3, pl.ds(8, 64), :] = IDS[...].astype(f32)

    for v in range(8):
        ci, h = v // 2, v % 2
        for k in range(4):
            x = HE[k, pl.ds(8 + 16 * ci + h, 8, stride=2), :]
            S1[pl.ds(ci * 128 + 2 * k + h, 8, stride=16), :] = swap_blocks(x, sub, lg)
    row32 = lax.broadcasted_iota(i32, (32, 32), 0)
    col32 = lax.broadcasted_iota(i32, (32, 32), 1)
    lane32 = lax.broadcasted_iota(i32, (32, 128), 1)
    box_rows = jnp.zeros((32, 128), f32)
    for k in range(4):
        one = jnp.broadcast_to(BOX[pl.ds(k, 1), :], (32, 32)).astype(f32)
        value = jnp.sum(jnp.where(row32 == col32, one, 0.0), axis=1, keepdims=True)
        box_rows = jnp.where(lane32 == k, value, box_rows)
    S1[pl.ds(8, 32, stride=16), :] = box_rows

    lane64 = lax.broadcasted_iota(i32, (64, 128), 1)
    packed = jnp.zeros((64, 128), f32)
    for k in range(4):
        near = (lane64 - 8 * k) & 127
        x = HE[k, pl.ds(8, 64), :]
        packed = jnp.where((near < 3) | (near >= 125), pltpu.roll(x, 8 * k, 1) if k else x, packed)
    PB[...] = packed

    TAB[pl.ds(0, 8), :] = jnp.ones((8, 128), f32)
    TAB[pl.ds(8, 8), :] = jnp.zeros((8, 128), f32)
    TAB[pl.ds(0, 8), pl.ds(0, 8)] = jnp.broadcast_to(EPS[...], (8, 8))
    TAB[pl.ds(8, 8), pl.ds(0, 8)] = jnp.broadcast_to(SIG[...], (8, 8))
    eps, sig = TAB[pl.ds(0, 8), :], TAB[pl.ds(8, 8), :]
    for j, table in enumerate(step_tables(eps, sig, 1.0) + step_tables(eps, sig, 3.0)):
        for k in range(8):
            TAB[pl.ds(16 + 64 * j + 8 * k, 8), :] = jnp.broadcast_to(table[:, k : k + 1], (8, 128))

    def table(j):
        return [TAB[pl.ds(16 + 64 * j + 8 * k, 8), :] for k in range(8)]

    damp1, gain1, damp3, gain3 = (functools.partial(table, j) for j in range(4))


    def put_coef(tg, u, ids):
        FD[cell_rows(tg, u), :] = pick(damp3(), ids)
        FG[cell_rows(tg, u), :] = pick(gain3(), ids)

    pl.semaphore_wait(barrier, 6 + (NB - 1) + 7 + 3)
    for n in y_peers:
        pl.semaphore_signal(stage_sem, inc=1, device_id=dev(n, b), device_id_type=MESH)

    halos = []

    def halo(j, src, dst, na, nb):
        copy = pltpu.make_async_remote_copy(
            src_ref=src, dst_ref=dst, send_sem=halo_send.at[j], recv_sem=halo_sem.at[j],
            device_id=dev(na, nb), device_id_type=MESH,
        )
        copy.start()
        halos.append(copy)

    halo(0, HE.at[:, pl.ds(64, 8), :], HE.at[:, pl.ds(0, 8), :], ap, b)
    halo(1, HE.at[:, pl.ds(8, 8), :], HE.at[:, pl.ds(72, 8), :], am, b)
    halo(2, PB, PEL.at[pl.ds(8, 64), :], a, bp)
    halo(3, PB, PER.at[pl.ds(8, 64), :], a, bm)
    halo(4, PB.at[pl.ds(56, 8), :], PEL.at[pl.ds(0, 8), :], ap, bp)
    halo(5, PB.at[pl.ds(56, 8), :], PER.at[pl.ds(0, 8), :], ap, bm)
    halo(6, PB.at[pl.ds(0, 8), :], PEL.at[pl.ds(72, 8), :], am, bp)
    halo(7, PB.at[pl.ds(0, 8), :], PER.at[pl.ds(72, 8), :], am, bm)

    def ring(d, size):
        return min(d, size - d)

    offsets = sorted(
        ((dy, dz) for dy in range(4) for dz in range(8) if dy or dz), key=lambda o: -(ring(o[0], 4) + ring(o[1], 8))
    )
    peers = [lax.rem(a // 8 + dy, 4) * 8 + lax.rem(lax.rem(a, 8) + dz, 8) for dy, dz in offsets]

    def exchange(j, src, dst, slot, rows, same=False):
        own = pl.multiple_of(a * slot, slot)
        for n in peers:
            pltpu.make_async_remote_copy(
                src_ref=src.at[pl.ds(0 if same else pl.multiple_of(n * slot, slot), rows), :],
                dst_ref=dst.at[pl.ds(own, rows), :],
                send_sem=send_sem.at[j], recv_sem=recv_sem.at[j],
                device_id=dev(n, b), device_id_type=MESH,
            ).start()
        dst[pl.ds(own, rows), :] = src[pl.ds(0 if same else own, rows), :]

    def received(j, buf, rows):
        total = (NA - 1) * rows
        return pltpu.make_async_copy(buf.at[pl.ds(0, total), :], buf.at[pl.ds(0, total), :], recv_sem.at[j])

    def sent(j, buf, rows):
        total = (NA - 1) * rows
        return pltpu.make_async_copy(buf.at[pl.ds(0, total), :], buf.at[pl.ds(0, total), :], send_sem.at[j])

    loads[4].wait()
    to_cells(FI, put_coef)
    pl.semaphore_wait(stage_sem, 3)
    exchange(0, S1, R1, 16, 9)

    loads[5].wait()
    to_cells(FE, put_in(WE))

    for copy in halos:
        copy.wait()
    lane80 = lax.broadcasted_iota(i32, (80, 128), 1)
    row80 = lax.broadcasted_iota(i32, (80, 128), 0)
    row_g = row80 + (a * 64 - 8)
    col_m = lane80 + b * 128
    col_s = jnp.where(lane80 < 64, col_m + 128, col_m - 128)
    row_ok = (row_g >= 0) & (row_g < NA * 64)
    ok_m = jnp.where(row_ok, 1.0, 0.0)
    ok_s = jnp.where(row_ok & (col_s >= 0) & (col_s < NB * 128), 1.0, 0.0)

    def sides(k):
        left, right = PEL[...], PER[...]
        if k:
            left, right = pltpu.roll(left, 128 - 8 * k, 1), pltpu.roll(right, 128 - 8 * k, 1)
        return jnp.where(lane80 >= 125, left, jnp.where(lane80 < 3, right, 0.0))

    pair_ez, pair_hx, pair_hy = ((HE[k] * ok_m, sides(k) * ok_s) for k in range(3))

    def coef80(table, ids, ok):
        parts = [pick(table, ids[8 * r : 8 * r + 8, :].astype(i32)) for r in range(10)]
        return jnp.concatenate(parts, axis=0) * ok

    ids_m, ids_s = HE[3], sides(3)
    pair_damp = (coef80(damp1(), ids_m, ok_m), coef80(damp1(), ids_s, ok_s))
    pair_gain = (coef80(gain1(), ids_m, ok_m), coef80(gain1(), ids_s, ok_s))

    def right_of(x):
        m, s = pltpu.roll(x[0], 127, 1), pltpu.roll(x[1], 127, 1)
        return jnp.where(lane80 < 127, m, s), jnp.where(lane80 < 127, s, m)

    def left_of(x):
        m, s = pltpu.roll(x[0], 1, 1), pltpu.roll(x[1], 1, 1)
        return jnp.where(lane80 >= 1, m, s), jnp.where(lane80 >= 1, s, m)

    def below(x):
        return pltpu.roll(x[0], 79, 0), pltpu.roll(x[1], 79, 0)

    def above(x):
        return pltpu.roll(x[0], 1, 0), pltpu.roll(x[1], 1, 0)

    def both(fn, *pairs):
        return tuple(fn(*(p[i] for p in pairs)) for i in range(2))

    src_i = [SRC[0, k] >> 10 for k in range(4)]
    src_j = [SRC[0, k] & 1023 for k in range(4)]

    def h_step(ez, hx, hy):
        hx = both(lambda h, e, r, k: (h - 0.5 * (r - e)) * k, hx, ez, right_of(ez), (ok_m, ok_s))
        hy = both(lambda h, e, r, k: (h + 0.5 * (r - e)) * k, hy, ez, below(ez), (ok_m, ok_s))
        return hx, hy

    for n in range(2):
        pair_hx, pair_hy = h_step(pair_ez, pair_hx, pair_hy)
        drive = []
        for col in (col_m, col_s):
            total = jnp.zeros((80, 128), f32)
            for k in range(4):
                total = total + jnp.where((row_g == src_i[k]) & (col == src_j[k]), WAVE[n, k], 0.0)
            drive.append(total)
        pair_ez = both(
            lambda d, e, g, hy, hu, hx, hl, s: d * e + g * ((hy - hu) - (hx - hl)) + s,
            pair_damp, pair_ez, pair_gain, pair_hy, above(pair_hy), pair_hx, left_of(pair_hx), tuple(drive),
        )
        E2[n] = pair_ez[0][8:72, :]
    pair_hx, pair_hy = h_step(pair_ez, pair_hx, pair_hy)
    E2[2] = jnp.where((row80 & 15) == 8, above(pair_hy)[0], pair_hy[0])[8:72, :]
    E2[3] = jnp.where((lane80 & 15) == 0, left_of(pair_hx)[0], pair_hx[0])[8:72, :]

    e4, t16 = (lane >> 4) & 3, lane & 15
    frame_idx = jnp.where(
        e4 == 0, t16,
        jnp.where(e4 == 1, 112 + t16, jnp.where(e4 == 2, 16 * (t16 >> 1), 16 * (t16 >> 1) + 15)),
    )
    from_h1 = jnp.where(e4 == 0, 0, jnp.where(e4 == 1, 1, t16 & 1)) == 1

    for ci in range(4):
        got = []
        for k in range(4):
            halves = []
            for h in range(2):
                x = E2[k, pl.ds(16 * ci + h, 8, stride=2), :]
                halves.append(lane_gather(swap_blocks(x, sub, lg), frame_idx))
            got.append(jnp.where(from_h1, halves[1], halves[0]))
        S2[pl.ds(ci * 64, 8, stride=8), :] = jnp.where(lane < 64, got[0], got[1])
        S2[pl.ds(ci * 64 + 1, 8, stride=8), :] = jnp.where((lane & 63) < 32, got[2], got[3])

    exchange(1, S2, R2, 8, 2)

    loads[6].wait()
    to_cells(FX, put_in(WX))
    loads[7].wait()
    to_cells(FY, put_in(WY))
    received(0, R1, 9).wait()

    def from1(k):
        return tuple(R1[pl.ds(2 * k + h, 32, stride=16), :] for h in range(2))

    ez, hx, hy, ids_c = (from1(k) for k in range(4))

    def coef32(table, ids):
        parts = [pick(table, ids[8 * r : 8 * r + 8, :].astype(i32)) for r in range(4)]
        return jnp.concatenate(parts, axis=0)

    damp = tuple(coef32(damp1(), x) for x in ids_c)
    gain = tuple(coef32(gain1(), x) for x in ids_c)
    rows_in = tuple(2 * (lane32 >> 4) + h for h in range(2))
    col_in = lane32 & 15
    boxes = R1[pl.ds(8, 32, stride=16), :]
    lo_i, lo_j, n_i, n_j = (jnp.broadcast_to(boxes[:, k : k + 1], (32, 128)).astype(i32) for k in range(4))
    mid = tuple((r > lo_i) & (r < lo_i + n_i - 1) & (col_in > lo_j) & (col_in < lo_j + n_j - 1) for r in rows_in)
    inbox = tuple((r >= lo_i) & (r < lo_i + n_i) & (col_in >= lo_j) & (col_in < lo_j + n_j) for r in rows_in)
    f_mid = tuple(jnp.where(m, 1.0, 0.0) for m in mid)
    f_in = tuple(jnp.where(m, 1.0, 0.0) for m in inbox)
    f_rim = both(lambda x, y: x - y, f_in, f_mid)
    for h in range(2):
        CO[0, pl.ds(32 * h, 32), :] = 0.5 * f_in[h]
        CO[4, pl.ds(32 * h, 32), :] = f_mid[h]

    def co_rows(tg, h):
        return pl.ds(pl.multiple_of(32 * h + 8 * tg, 8), 8)

    def prepare(tg, carry):
        halves = [(2.0 * CO[0, co_rows(tg, h), :], CO[4, co_rows(tg, h), :]) for h in range(2)]
        for u in range(18):
            box, middle = halves[u // 9]
            rows = cell_rows(tg, u)
            WX[rows, :] = WX[rows, :] * box
            WY[rows, :] = WY[rows, :] * box
            FD[rows, :] = FD[rows, :] * middle
            FG[rows, :] = FG[rows, :] * middle
        return carry

    lax.fori_loop(0, 4, prepare, 0)

    def substep(k, carry):
        m, tg = k // 4, lax.rem(k, 4)
        half_box = [CO[0, co_rows(tg, h), :] for h in range(2)]
        rim = [CO[1 + m, co_rows(tg, h), :] for h in range(2)]
        e = [WE[cell_rows(tg, u), :] for u in range(18)]
        x, y = [None] * 18, [None] * 18

        def magnetic(p):
            for u in range(3 * p, 3 * p + 3):
                c = half_box[u // 9]
                after = e[u + 1] if u % 3 < 2 else pltpu.roll(e[u - 2], 127, 1)
                under = e[u + 3] if u < 15 else pltpu.roll(e[u - 15], 112, 1)
                x[u] = WX[cell_rows(tg, u), :] - c * (after - e[u])
                y[u] = WY[cell_rows(tg, u), :] + c * (under - e[u])
                WX[cell_rows(tg, u), :] = x[u]
                WY[cell_rows(tg, u), :] = y[u]

        def electric(p):
            for u in range(3 * p, 3 * p + 3):
                before = x[u - 1] if u % 3 else pltpu.roll(x[u + 2], 1, 1)
                over = y[u - 3] if u >= 3 else pltpu.roll(y[u + 15], 16, 1)
                curl = (y[u] - over) - (x[u] - before)
                WE[cell_rows(tg, u), :] = (
                    FD[cell_rows(tg, u), :] * e[u] + FG[cell_rows(tg, u), :] * curl + rim[u // 9]
                )

        magnetic(5)
        magnetic(0)
        for p in range(1, 5):
            magnetic(p)
            electric(p - 1)
        electric(4)
        electric(5)
        return carry

    def means(tg, carry):
        for h in range(2):
            part = [WE[cell_rows(tg, u), :] for u in range(9 * h, 9 * h + 9)]
            total = ((part[0] + part[1]) + (part[2] + part[3])) + ((part[4] + part[5]) + (part[6] + part[7])) + part[8]
            CO[5, co_rows(tg, h), :] = total * (1.0 / 9.0)
        return carry

    edge_col = (col_in == 0) | (col_in == 15)
    frame = (edge_col | (rows_in[0] == 0), edge_col | (rows_in[1] == 15))
    tile32 = lax.broadcasted_iota(i32, (32, 128), 0)
    my_ci, my_cj = a // 8, lax.rem(a, 8)
    src_tile, src_cell = [], []
    for k in range(4):
        i, j = src_i[k], src_j[k]
        here = ((i & 63) >> 4 == my_ci) & ((j & 127) >> 4 == my_cj) & (j >> 7 == b)
        src_tile.append(jnp.where(here, i >> 6, -1))
        src_cell.append((i & 1) * 128 + ((i & 15) >> 1) * 16 + (j & 15))
    rcv = jnp.broadcast_to(RCV[...], (8, 128))
    ri, rj = rcv >> 10, rcv & 1023
    r_here = (((ri & 63) >> 4) == my_ci) & (((rj & 127) >> 4) == my_cj) & ((rj >> 7) == b)
    r_tile = jnp.where(r_here, ri >> 6, -1)
    r_idx, r_half = ((ri & 15) >> 1) * 16 + (rj & 15), ri & 1

    def c_right(x):
        return tuple(pltpu.roll(v, 127, 1) for v in x)

    def c_left(x):
        return tuple(pltpu.roll(v, 1, 1) for v in x)

    def c_below(x):
        return x[1], pltpu.roll(x[0], 112, 1)

    def c_above(x):
        return pltpu.roll(x[1], 16, 1), x[0]

    for n in range(STEPS):
        hx = both(lambda h, e, r: h - 0.5 * (r - e), hx, ez, c_right(ez))
        hy = both(lambda h, e, r: h + 0.5 * (r - e), hy, ez, c_below(ez))
        hx_left, hy_up = c_left(hx), c_above(hy)
        if n == 2:
            edge = R2[pl.ds(1, 32, stride=8), :]

            def spread(idx):
                parts = [lane_gather(edge[8 * r : 8 * r + 8, :], idx) for r in range(4)]
                return jnp.concatenate(parts, axis=0)

            w1 = tuple(spread(t16 + 16 * h) for h in range(2))
            w2 = tuple(spread(jnp.where(t16 == 15, 48, 32) + 2 * (lane >> 4) + h) for h in range(2))
            hy = (hy[0], jnp.where(rows_in[1] == 15, w1[1], hy[1]))
            hx = tuple(jnp.where(col_in == 15, w2[h], hx[h]) for h in range(2))
            hy_up = (jnp.where(rows_in[0] == 0, w1[0], hy_up[0]), hy_up[1])
            hx_left = tuple(jnp.where(col_in == 0, w2[h], hx_left[h]) for h in range(2))
            for h in range(2):
                O1[pl.ds(h, 32, stride=8), :] = hx[h]
                O1[pl.ds(2 + h, 32, stride=8), :] = hy[h]
            exchange(2, O1, RO1, 8, 4)
        drive = []
        for h in range(2):
            total = jnp.zeros((32, 128), f32)
            for k in range(4):
                total = total + jnp.where(
                    (tile32 == src_tile[k]) & (lane32 + 128 * h == src_cell[k]), WAVE[n, k], 0.0
                )
            drive.append(total)
        new = both(
            lambda d, e, g, y, yu, x, xl, s: d * e + g * ((y - yu) - (x - xl)) + s,
            damp, ez, gain, hy, hy_up, hx, hx_left, tuple(drive),
        )
        for m in range(3):
            share = (m + 1) / 3.0
            for h in range(2):
                CO[1 + m, pl.ds(32 * h, 32), :] = f_rim[h] * ((1.0 - share) * ez[h] + share * new[h])
        lax.fori_loop(0, 12, substep, 0)
        lax.fori_loop(0, 4, means, 0)
        if n == 0:
            received(1, R2, 2).wait()
        if n < 2:
            rim = R2[pl.ds(0, 32, stride=8), :]
            out = []
            for h in range(2):
                r = 2 * (lane >> 4) + h
                slot = jnp.where(
                    r == 0, t16, jnp.where(r == 15, 16 + t16, jnp.where(t16 == 0, 32 + r, 48 + r))
                )
                slot = (slot & 63) + 64 * n
                parts = [lane_gather(rim[8 * q : 8 * q + 8, :], slot) for q in range(4)]
                out.append(jnp.where(frame[h], jnp.concatenate(parts, axis=0), new[h]))
            new = tuple(out)
        ez = both(lambda m, x, y: jnp.where(m, x, y), mid, (CO[5, pl.ds(0, 32), :], CO[5, pl.ds(32, 32), :]), new)
        picked = jnp.zeros((8, 128), f32)
        for h in range(2):
            for q in range(4):
                got = lane_gather(ez[h][8 * q : 8 * q + 8, :], r_idx)
                picked = picked + jnp.where((r_tile == sub + 8 * q) & (r_half == h), got, 0.0)
        TS[pl.ds(n, 1), :] = jnp.sum(picked, axis=0, keepdims=True)

    for d in range(1, NB):
        n = lax.rem(b + d, NB)
        pltpu.make_async_remote_copy(
            src_ref=TS.at[pl.ds(0, 3), :],
            dst_ref=TB.at[pl.ds(pl.multiple_of(8 * b, 8), 3), :],
            send_sem=send_sem.at[4], recv_sem=recv_sem.at[4],
            device_id=dev(a, n), device_id_type=MESH,
        ).start()
    TB[pl.ds(pl.multiple_of(8 * b, 8), 3), :] = TS[pl.ds(0, 3), :]

    for h in range(2):
        O2[pl.ds(h, 32, stride=8), :] = ez[h]
    exchange(3, O2, RO2, 8, 2)

    from_cells(WE, FE)
    from_cells(WX, FX)
    seven = (NB - 1) * 3
    pltpu.make_async_copy(TB.at[pl.ds(0, seven), :], TB.at[pl.ds(0, seven), :], recv_sem.at[4]).wait()
    for n in range(STEPS):
        TS2[pl.ds(n, 1), :] = jnp.sum(TB[pl.ds(n, 8, stride=8), :], axis=0, keepdims=True)
    exchange(5, TS2, TG, 8, 3, same=True)

    from_cells(WY, FY)
    received(2, RO1, 4).wait()

    def unpack(src, first, dst):
        for ci in range(4):
            for h in range(2):
                x = src[pl.ds(ci * 64 + first + h, 8, stride=8), :]
                dst[pl.ds(16 * ci + h, 8, stride=2), :] = swap_blocks(x, sub, lg)

    unpack(RO1, 0, hx_out)
    unpack(RO1, 2, hy_out)
    received(3, RO2, 2).wait()
    unpack(RO2, 0, ez_out)
    received(5, TG, 3).wait()
    for n in range(STEPS):
        tr_out[pl.ds(n, 1), :] = jnp.sum(TG[pl.ds(n, 32, stride=8), :], axis=0, keepdims=True)

    for j, buf, rows in ((0, S1, 9), (1, S2, 2), (2, O1, 4), (3, O2, 2), (5, TG, 3)):
        sent(j, buf, rows).wait()
    pltpu.make_async_copy(TB.at[pl.ds(0, seven), :], TB.at[pl.ds(0, seven), :], send_sem.at[4]).wait()


def finish(*refs):
    sources, outs, sems = refs[:7], refs[7:14], refs[14]
    copies = [pltpu.make_async_copy(x, y, sems.at[j]) for j, (x, y) in enumerate(zip(sources, outs))]
    for copy in copies:
        copy.start()
    for copy in copies:
        copy.wait()


def shards(
    coarse_ez, coarse_hx, coarse_hy, coarse_ids, mat_eps, mat_sig,
    fine_ez, fine_hx, fine_hy, fine_ids, boxes, src_cells, src_wave, rcv_cells,
):
    fine_shape = fine_ez.shape
    flat = (576, 128)
    anywhere = pl.BlockSpec(memory_space=pl.ANY)
    vmem = pl.BlockSpec(memory_space=pltpu.VMEM)
    shapes = ((64, 128),) * 3 + (flat,) * 3 + ((3, 128),)

    def v(*shape, dtype=f32):
        return pltpu.VMEM(shape, dtype)

    def dma(n):
        return pltpu.SemaphoreType.DMA((n,))

    outs = pl.pallas_call(
        kernel,
        name="nested",
        out_shape=tuple(pltpu.VMEM(shape, f32) for shape in shapes),
        in_specs=[anywhere] * 14,
        out_specs=(vmem,) * 7,
        scratch_shapes=[
            v(4, 80, 128), v(64, 128, dtype=i32), v(64, 128), v(80, 128), v(80, 128), v(4, 64, 128),
            v(512, 128), v(512, 128), v(256, 128), v(256, 128),
            v(256, 128), v(256, 128), v(256, 128), v(256, 128),
            v(8, 128), v(64, 128), v(8, 128), v(256, 128),
            v(576, 128, dtype=i32), v(584, 128), v(584, 128),
            v(584, 128), v(584, 128), v(584, 128),
            v(144, 128, dtype=i32), v(144, 128, dtype=i32), v(272, 128), v(6, 64, 128),
            v(4, 32, dtype=i32), pltpu.SMEM((1, 4), i32), pltpu.SMEM((3, 4), f32),
            v(1, 128, dtype=i32), v(1, 8), v(1, 8),
            dma(14), dma(8), dma(8), dma(6), dma(6), pltpu.SemaphoreType.REGULAR,
        ],
        compiler_params=pltpu.CompilerParams(collective_id=0, has_side_effects=True),
    )(
        coarse_ez, coarse_hx, coarse_hy, coarse_ids,
        mat_eps.reshape(1, 8), mat_sig.reshape(1, 8),
        fine_ez.reshape(flat), fine_hx.reshape(flat), fine_hy.reshape(flat), fine_ids.reshape(flat),
        boxes.reshape(32, 4).T, src_cells.reshape(1, 4), src_wave, rcv_cells.reshape(1, 128),
    )
    outs = pl.pallas_call(
        finish,
        name="finish",
        out_shape=tuple(jax.ShapeDtypeStruct(shape, f32) for shape in shapes),
        in_specs=[vmem] * 7,
        out_specs=(anywhere,) * 7,
        scratch_shapes=[dma(7)],
    )(*(pltpu.with_memory_space_constraint(x, pltpu.VMEM) for x in outs))
    return tuple(outs[:3]) + tuple(x.reshape(fine_shape) for x in outs[3:6]) + (outs[6],)


def solution(mesh):
    coarse = P("gx", ("grp", "gy"))
    tiles = P(None, ("grp", "gy"), "gx", None)
    in_specs = (
        coarse, coarse, coarse, coarse, P(), P(), tiles, tiles, tiles, tiles,
        P("gx", ("grp", "gy"), None, None), P(), P(), P(),
    )
    out_specs = (coarse, coarse, coarse, tiles, tiles, tiles, P())
    return jax.shard_map(shards, mesh=mesh, in_specs=in_specs, out_specs=out_specs, check_vma=False)
```

```python
import functools

import jax
import jax.numpy as jnp
from jax import lax
from jax.experimental import pallas as pl
from jax.experimental.pallas import tpu as pltpu
from jax.sharding import PartitionSpec as P

MESH = pl.DeviceIdType.MESH
NA = 32
NB = 8
STEPS = 3
f32 = jnp.float32
i32 = jnp.int32


def lanes():
    return lax.broadcasted_iota(i32, (8, 128), 1)


def sublanes():
    return lax.broadcasted_iota(i32, (8, 128), 0)


def swap_blocks(x, sub, lg):
    for k in range(3):
        bs = (sub >> k) & 1
        bl = (lg >> k) & 1
        step = 16 << k
        down = pltpu.roll(pltpu.roll(x, 1 << k, 0), 128 - step, 1)
        up = pltpu.roll(pltpu.roll(x, 8 - (1 << k), 0), step, 1)
        x = jnp.where(bs == bl, x, jnp.where(bs == 1, down, up))
    return x


def lane_gather(x, idx):
    return jnp.take_along_axis(x, idx, axis=1)


def div(x, n):
    return (x * ((1 << 20) // n + 1)) >> 20


FINE = 48


def sources_of_cells():
    need = [set() for _ in range(18)]
    back = [set() for _ in range(18)]
    for p in range(FINE):
        for q in range(FINE):
            u, g = 3 * (p % 6) + q % 3, (p * FINE + q) // 128
            need[u].add(g)
            back[g].add(u)
    return [sorted(x) for x in need], [sorted(x) for x in back]


NEED, BACK = sources_of_cells()


def pick(table, ids):
    bits = [(ids & (1 << k)) != 0 for k in range(3)]
    for bit in bits:
        table = [jnp.where(bit, table[i + 1], table[i]) for i in range(0, len(table), 2)]
    return table[0]


def step_tables(eps, sig, ratio):
    loss = sig / (eps * ratio)
    return (1.0 - loss) / (1.0 + loss), 0.5 / (eps * (1.0 + loss))


def kernel(
    ez_in, hx_in, hy_in, ids_in, eps_in, sig_in, fez_in, fhx_in, fhy_in, fids_in, box_in, src_in, wave_in, rcv_in,
    ez_out, hx_out, hy_out, fez_out, fhx_out, fhy_out, tr_out,
    HE, DG, IDS, PB, PEL, PER, E2, S1, R1, S2, R2, O1, RO1, TS, TB, TS2, TG,
    FI, FD, FG, WE, WX, WY, IDX, SEL, TAB, CO, BOX, SRC, WAVE, RCV, EPS, SIG,
    MANY, in_sem, halo_sem, send_sem, recv_sem, stage_sem,
):
    FE, FX, FY = fez_out, fhx_out, fhy_out
    grp = lax.axis_index("grp")
    a = lax.axis_index("gx")
    gy = lax.axis_index("gy")
    b = grp * 4 + gy

    def dev(na, nb):
        return (nb // 4, na, nb % 4)

    am, ap = lax.rem(a + NA - 1, NA), lax.rem(a + 1, NA)
    bm, bp = lax.rem(b + NB - 1, NB), lax.rem(b + 1, NB)

    def bytes_of(rows, sem):
        return pltpu.make_async_copy(MANY.at[pl.ds(0, rows), :], MANY.at[pl.ds(0, rows), :], sem)

    loads = []
    for j, (source, dst) in enumerate((
        (ez_in, HE.at[0, pl.ds(8, 64), :]),
        (hx_in, HE.at[1, pl.ds(8, 64), :]),
        (hy_in, HE.at[2, pl.ds(8, 64), :]),
        (ids_in, IDS),
        (fids_in, FI),
        (fez_in, FE),
        (fhx_in, FX),
        (fhy_in, FY),
        (box_in, BOX),
        (eps_in, EPS),
        (sig_in, SIG),
        (rcv_in, RCV),
        (src_in, SRC),
        (wave_in, WAVE),
    )):
        copy = pltpu.make_async_copy(source, dst, in_sem.at[min(j // 4, 2) + max(j - 8, 0)])
        copy.start()
        loads.append(copy)

    barrier = pltpu.get_barrier_semaphore()

    def signal(na, nb):
        pl.semaphore_signal(barrier, inc=1, device_id=dev(na, nb), device_id_type=MESH)

    y, z = a // 8, lax.rem(a, 8)
    for na in (am, ap):
        for nb in (bm, b, bp):
            signal(na, nb)
    for d in range(1, NB):
        signal(a, lax.rem(b + d, NB))
    for d in range(1, 8):
        signal(y * 8 + lax.rem(z + d, 8), b)
    y_peers = [lax.rem(y + d, 4) * 8 + z for d in range(1, 4)]
    for n in y_peers:
        signal(n, b)

    lane = lanes()
    sub = sublanes()
    lg = lane >> 4

    for g in range(18):
        pos = lane + 128 * g
        p = div(pos, 48)
        q = pos - 48 * p
        pb, j = div(p, 6), div(q, 3)
        IDX[pl.ds(8 * g, 8), :] = 16 * pb + j
        SEL[pl.ds(8 * g, 8), :] = 3 * (p - 6 * pb) + (q - 3 * j)
    cell_pos = 288 * (lane >> 4) + 3 * (lane & 15)

    def flat_rows(tg, g):
        return pl.ds(tg * 144 + g, 8, stride=18)

    def aligned(start, size):
        return pl.ds(start if isinstance(start, int) else pl.multiple_of(start, 8), size)

    def cell_rows(tg, u):
        return aligned(tg * 144 + 8 * u, 8)

    def each_pair(body):
        def pair(half, carry):
            for k in range(2):
                body(2 * half + k)
            return carry

        lax.fori_loop(0, 2, pair, 0)

    def to_cells(src, put):
        def body(tg):
            flat = [src[flat_rows(tg, g), :] for g in range(18)]
            for u in range(18):
                pos = cell_pos + (48 * (u // 3) + u % 3)
                idx, group = pos & 127, pos >> 7
                value = lane_gather(flat[NEED[u][0]], idx)
                for g in NEED[u][1:]:
                    value = jnp.where(group == g, lane_gather(flat[g], idx), value)
                put(tg, u, value)

        each_pair(body)

    def put_in(dst):
        def put(tg, u, value):
            dst[cell_rows(tg, u), :] = value

        return put

    def from_cells(src, dst):
        def body(tg):
            cells = [src[cell_rows(tg, u), :] for u in range(18)]
            for g in range(18):
                idx, group = IDX[pl.ds(8 * g, 8), :], SEL[pl.ds(8 * g, 8), :]
                value = lane_gather(cells[BACK[g][0]], idx)
                for u in BACK[g][1:]:
                    value = jnp.where(group == u, lane_gather(cells[u], idx), value)
                dst[flat_rows(tg, g), :] = value

        each_pair(body)

    bytes_of(4 * 64, in_sem.at[0]).wait()
    for copy in loads[8:]:
        copy.wait()
    HE[3, pl.ds(8, 64), :] = IDS[...].astype(f32)

    for v in range(8):
        ci, h = v // 2, v % 2
        for k in range(4):
            x = HE[k, pl.ds(8 + 16 * ci + h, 8, stride=2), :]
            S1[pl.ds(ci * 128 + 2 * k + h, 8, stride=16), :] = swap_blocks(x, sub, lg)
    row32 = lax.broadcasted_iota(i32, (32, 32), 0)
    col32 = lax.broadcasted_iota(i32, (32, 32), 1)
    lane32 = lax.broadcasted_iota(i32, (32, 128), 1)
    box_rows = jnp.zeros((32, 128), f32)
    for k in range(4):
        one = jnp.broadcast_to(BOX[pl.ds(k, 1), :], (32, 32)).astype(f32)
        value = jnp.sum(jnp.where(row32 == col32, one, 0.0), axis=1, keepdims=True)
        box_rows = jnp.where(lane32 == k, value, box_rows)
    S1[pl.ds(8, 32, stride=16), :] = box_rows

    lane64 = lax.broadcasted_iota(i32, (64, 128), 1)
    packed = jnp.zeros((64, 128), f32)
    for k in range(4):
        near = (lane64 - 8 * k) & 127
        x = HE[k, pl.ds(8, 64), :]
        packed = jnp.where((near < 3) | (near >= 125), pltpu.roll(x, 8 * k, 1) if k else x, packed)
    PB[...] = packed

    TAB[pl.ds(0, 8), :] = jnp.ones((8, 128), f32)
    TAB[pl.ds(8, 8), :] = jnp.zeros((8, 128), f32)
    TAB[pl.ds(0, 8), pl.ds(0, 8)] = jnp.broadcast_to(EPS[...], (8, 8))
    TAB[pl.ds(8, 8), pl.ds(0, 8)] = jnp.broadcast_to(SIG[...], (8, 8))
    eps, sig = TAB[pl.ds(0, 8), :], TAB[pl.ds(8, 8), :]
    for j, table in enumerate(step_tables(eps, sig, 1.0) + step_tables(eps, sig, 3.0)):
        for k in range(8):
            TAB[pl.ds(16 + 64 * j + 8 * k, 8), :] = jnp.broadcast_to(table[:, k : k + 1], (8, 128))

    def table(j):
        return [TAB[pl.ds(16 + 64 * j + 8 * k, 8), :] for k in range(8)]

    damp1, gain1, damp3, gain3 = (functools.partial(table, j) for j in range(4))


    def put_coef(tg, u, ids):
        FD[cell_rows(tg, u), :] = pick(damp3(), ids)
        FG[cell_rows(tg, u), :] = pick(gain3(), ids)

    pl.semaphore_wait(barrier, 6 + (NB - 1) + 7 + 3)
    for n in y_peers:
        pl.semaphore_signal(stage_sem, inc=1, device_id=dev(n, b), device_id_type=MESH)

    def halo(src, dst, na, nb):
        copy = pltpu.make_async_remote_copy(
            src_ref=src, dst_ref=dst, send_sem=send_sem, recv_sem=halo_sem,
            device_id=dev(na, nb), device_id_type=MESH,
        )
        copy.start()

    halo(HE.at[:, pl.ds(64, 8), :], HE.at[:, pl.ds(0, 8), :], ap, b)
    halo(HE.at[:, pl.ds(8, 8), :], HE.at[:, pl.ds(72, 8), :], am, b)
    halo(PB, PEL.at[pl.ds(8, 64), :], a, bp)
    halo(PB, PER.at[pl.ds(8, 64), :], a, bm)
    halo(PB.at[pl.ds(56, 8), :], PEL.at[pl.ds(0, 8), :], ap, bp)
    halo(PB.at[pl.ds(56, 8), :], PER.at[pl.ds(0, 8), :], ap, bm)
    halo(PB.at[pl.ds(0, 8), :], PEL.at[pl.ds(72, 8), :], am, bp)
    halo(PB.at[pl.ds(0, 8), :], PER.at[pl.ds(72, 8), :], am, bm)

    def ring(d, size):
        return min(d, size - d)

    offsets = sorted(
        ((dy, dz) for dy in range(4) for dz in range(8) if dy or dz), key=lambda o: -(ring(o[0], 4) + ring(o[1], 8))
    )
    peers = [lax.rem(a // 8 + dy, 4) * 8 + lax.rem(lax.rem(a, 8) + dz, 8) for dy, dz in offsets]

    def exchange(j, src, dst, slot, rows, same=False):
        own = pl.multiple_of(a * slot, slot)
        for n in peers:
            pltpu.make_async_remote_copy(
                src_ref=src.at[pl.ds(0 if same else pl.multiple_of(n * slot, slot), rows), :],
                dst_ref=dst.at[pl.ds(own, rows), :],
                send_sem=send_sem, recv_sem=recv_sem.at[j],
                device_id=dev(n, b), device_id_type=MESH,
            ).start()
        dst[pl.ds(own, rows), :] = src[pl.ds(0 if same else own, rows), :]

    def received(j, rows):
        return bytes_of((NA - 1) * rows, recv_sem.at[j])

    bytes_of(4 * 576, in_sem.at[1]).wait()
    to_cells(FI, put_coef)
    pl.semaphore_wait(stage_sem, 3)
    exchange(0, S1, R1, 16, 9)

    def coef_rows(ids):
        ids = ids.astype(i32)
        return pick(damp1(), ids), pick(gain1(), ids)

    for r in range(1, 9):
        DG[0, pl.ds(8 * r, 8), :], DG[1, pl.ds(8 * r, 8), :] = coef_rows(HE[3, pl.ds(8 * r, 8), :])
    bytes_of(2 * 32 + 2 * 64 + 4 * 8, halo_sem).wait()
    for r in (0, 9):
        DG[0, pl.ds(8 * r, 8), :], DG[1, pl.ds(8 * r, 8), :] = coef_rows(HE[3, pl.ds(8 * r, 8), :])
    lane80 = lax.broadcasted_iota(i32, (80, 128), 1)
    row80 = lax.broadcasted_iota(i32, (80, 128), 0)
    row_g = row80 + (a * 64 - 8)
    col_m = lane80 + b * 128
    col_s = jnp.where(lane80 < 64, col_m + 128, col_m - 128)
    row_ok = (row_g >= 0) & (row_g < NA * 64)
    ok_m = jnp.where(row_ok, 1.0, 0.0)
    ok_s = jnp.where(row_ok & (col_s >= 0) & (col_s < NB * 128), 1.0, 0.0)

    def sides(k):
        left, right = PEL[...], PER[...]
        if k:
            left, right = pltpu.roll(left, 128 - 8 * k, 1), pltpu.roll(right, 128 - 8 * k, 1)
        return jnp.where(lane80 >= 125, left, jnp.where(lane80 < 3, right, 0.0))

    pair_ez, pair_hx, pair_hy = ((HE[k] * ok_m, sides(k) * ok_s) for k in range(3))

    ids_s = sides(3)
    sides_dg = [coef_rows(ids_s[8 * r : 8 * r + 8, :]) for r in range(10)]
    pair_damp, pair_gain = (
        (DG[k] * ok_m, jnp.concatenate([part[k] for part in sides_dg], axis=0) * ok_s) for k in range(2)
    )

    def right_of(x):
        m, s = pltpu.roll(x[0], 127, 1), pltpu.roll(x[1], 127, 1)
        return jnp.where(lane80 < 127, m, s), jnp.where(lane80 < 127, s, m)

    def left_of(x):
        m, s = pltpu.roll(x[0], 1, 1), pltpu.roll(x[1], 1, 1)
        return jnp.where(lane80 >= 1, m, s), jnp.where(lane80 >= 1, s, m)

    def below(x):
        return pltpu.roll(x[0], 79, 0), pltpu.roll(x[1], 79, 0)

    def above(x):
        return pltpu.roll(x[0], 1, 0), pltpu.roll(x[1], 1, 0)

    def both(fn, *pairs):
        return tuple(fn(*(p[i] for p in pairs)) for i in range(2))

    src_i = [SRC[0, k] >> 10 for k in range(4)]
    src_j = [SRC[0, k] & 1023 for k in range(4)]

    def h_step(ez, hx, hy):
        hx = both(lambda h, e, r, k: (h - 0.5 * (r - e)) * k, hx, ez, right_of(ez), (ok_m, ok_s))
        hy = both(lambda h, e, r, k: (h + 0.5 * (r - e)) * k, hy, ez, below(ez), (ok_m, ok_s))
        return hx, hy

    for n in range(2):
        pair_hx, pair_hy = h_step(pair_ez, pair_hx, pair_hy)
        drive = []
        for col in (col_m, col_s):
            total = jnp.zeros((80, 128), f32)
            for k in range(4):
                total = total + jnp.where((row_g == src_i[k]) & (col == src_j[k]), WAVE[n, k], 0.0)
            drive.append(total)
        pair_ez = both(
            lambda d, e, g, hy, hu, hx, hl, s: d * e + g * ((hy - hu) - (hx - hl)) + s,
            pair_damp, pair_ez, pair_gain, pair_hy, above(pair_hy), pair_hx, left_of(pair_hx), tuple(drive),
        )
        E2[n] = pair_ez[0][8:72, :]
    pair_hx, pair_hy = h_step(pair_ez, pair_hx, pair_hy)
    E2[2] = jnp.where((row80 & 15) == 8, above(pair_hy)[0], pair_hy[0])[8:72, :]
    E2[3] = jnp.where((lane80 & 15) == 0, left_of(pair_hx)[0], pair_hx[0])[8:72, :]

    e4, t16 = (lane >> 4) & 3, lane & 15
    frame_idx = jnp.where(
        e4 == 0, t16,
        jnp.where(e4 == 1, 112 + t16, jnp.where(e4 == 2, 16 * (t16 >> 1), 16 * (t16 >> 1) + 15)),
    )
    from_h1 = jnp.where(e4 == 0, 0, jnp.where(e4 == 1, 1, t16 & 1)) == 1

    for ci in range(4):
        got = []
        for k in range(4):
            halves = []
            for h in range(2):
                x = E2[k, pl.ds(16 * ci + h, 8, stride=2), :]
                halves.append(lane_gather(swap_blocks(x, sub, lg), frame_idx))
            got.append(jnp.where(from_h1, halves[1], halves[0]))
        S2[pl.ds(ci * 64, 8, stride=8), :] = jnp.where(lane < 64, got[0], got[1])
        S2[pl.ds(ci * 64 + 1, 8, stride=8), :] = jnp.where((lane & 63) < 32, got[2], got[3])

    exchange(1, S2, R2, 8, 2)

    to_cells(FE, put_in(WE))
    to_cells(FX, put_in(WX))
    to_cells(FY, put_in(WY))
    received(0, 9).wait()

    def from1(k):
        return tuple(R1[pl.ds(2 * k + h, 32, stride=16), :] for h in range(2))

    ez, hx, hy, ids_c = (from1(k) for k in range(4))

    def coef32(table, ids):
        parts = [pick(table, ids[8 * r : 8 * r + 8, :].astype(i32)) for r in range(4)]
        return jnp.concatenate(parts, axis=0)

    damp = tuple(coef32(damp1(), x) for x in ids_c)
    gain = tuple(coef32(gain1(), x) for x in ids_c)
    rows_in = tuple(2 * (lane32 >> 4) + h for h in range(2))
    col_in = lane32 & 15
    boxes = R1[pl.ds(8, 32, stride=16), :]
    lo_i, lo_j, n_i, n_j = (jnp.broadcast_to(boxes[:, k : k + 1], (32, 128)).astype(i32) for k in range(4))
    mid = tuple((r > lo_i) & (r < lo_i + n_i - 1) & (col_in > lo_j) & (col_in < lo_j + n_j - 1) for r in rows_in)
    inbox = tuple((r >= lo_i) & (r < lo_i + n_i) & (col_in >= lo_j) & (col_in < lo_j + n_j) for r in rows_in)
    f_mid = tuple(jnp.where(m, 1.0, 0.0) for m in mid)
    f_in = tuple(jnp.where(m, 1.0, 0.0) for m in inbox)
    f_rim = both(lambda x, y: x - y, f_in, f_mid)
    for h in range(2):
        CO[0, pl.ds(32 * h, 32), :] = 0.5 * f_in[h]
        CO[4, pl.ds(32 * h, 32), :] = f_mid[h]

    def co_rows(tg, h):
        return aligned(32 * h + 8 * tg, 8)

    def prepare(tg, carry):
        halves = [(2.0 * CO[0, co_rows(tg, h), :], CO[4, co_rows(tg, h), :]) for h in range(2)]
        for u in range(18):
            box, middle = halves[u // 9]
            rows = cell_rows(tg, u)
            WX[rows, :] = WX[rows, :] * box
            WY[rows, :] = WY[rows, :] * box
            FD[rows, :] = FD[rows, :] * middle
            FG[rows, :] = FG[rows, :] * middle
        return carry

    lax.fori_loop(0, 4, prepare, 0)

    def substeps(m, carry):
        for tg in range(4):
            substep(m, tg)
        return carry

    def substep(m, tg):
        half_box = [CO[0, co_rows(tg, h), :] for h in range(2)]
        rim = [CO[1 + m, co_rows(tg, h), :] for h in range(2)]
        e = [WE[cell_rows(tg, u), :] for u in range(18)]
        x, y = [None] * 18, [None] * 18

        def magnetic(p):
            for u in range(3 * p, 3 * p + 3):
                c = half_box[u // 9]
                after = e[u + 1] if u % 3 < 2 else pltpu.roll(e[u - 2], 127, 1)
                under = e[u + 3] if u < 15 else pltpu.roll(e[u - 15], 112, 1)
                x[u] = WX[cell_rows(tg, u), :] - c * (after - e[u])
                y[u] = WY[cell_rows(tg, u), :] + c * (under - e[u])
                WX[cell_rows(tg, u), :] = x[u]
                WY[cell_rows(tg, u), :] = y[u]

        def electric(p):
            for u in range(3 * p, 3 * p + 3):
                before = x[u - 1] if u % 3 else pltpu.roll(x[u + 2], 1, 1)
                over = y[u - 3] if u >= 3 else pltpu.roll(y[u + 15], 16, 1)
                curl = (y[u] - over) - (x[u] - before)
                WE[cell_rows(tg, u), :] = (
                    FD[cell_rows(tg, u), :] * e[u] + FG[cell_rows(tg, u), :] * curl + rim[u // 9]
                )

        magnetic(5)
        magnetic(0)
        for p in range(1, 5):
            magnetic(p)
            electric(p - 1)
        electric(4)
        electric(5)

    def means(tg):
        for h in range(2):
            part = [WE[cell_rows(tg, u), :] for u in range(9 * h, 9 * h + 9)]
            total = ((part[0] + part[1]) + (part[2] + part[3])) + ((part[4] + part[5]) + (part[6] + part[7])) + part[8]
            CO[5, co_rows(tg, h), :] = total * (1.0 / 9.0)

    edge_col = (col_in == 0) | (col_in == 15)
    frame = (edge_col | (rows_in[0] == 0), edge_col | (rows_in[1] == 15))
    tile32 = lax.broadcasted_iota(i32, (32, 128), 0)
    my_ci, my_cj = a // 8, lax.rem(a, 8)
    src_tile, src_cell = [], []
    for k in range(4):
        i, j = src_i[k], src_j[k]
        here = ((i & 63) >> 4 == my_ci) & ((j & 127) >> 4 == my_cj) & (j >> 7 == b)
        src_tile.append(jnp.where(here, i >> 6, -1))
        src_cell.append((i & 1) * 128 + ((i & 15) >> 1) * 16 + (j & 15))
    rcv = jnp.broadcast_to(RCV[...], (8, 128))
    ri, rj = rcv >> 10, rcv & 1023
    r_here = (((ri & 63) >> 4) == my_ci) & (((rj & 127) >> 4) == my_cj) & ((rj >> 7) == b)
    r_tile = jnp.where(r_here, ri >> 6, -1)
    r_idx, r_half = ((ri & 15) >> 1) * 16 + (rj & 15), ri & 1

    def c_right(x):
        return tuple(pltpu.roll(v, 127, 1) for v in x)

    def c_left(x):
        return tuple(pltpu.roll(v, 1, 1) for v in x)

    def c_below(x):
        return x[1], pltpu.roll(x[0], 112, 1)

    def c_above(x):
        return pltpu.roll(x[1], 16, 1), x[0]

    for n in range(STEPS):
        hx = both(lambda h, e, r: h - 0.5 * (r - e), hx, ez, c_right(ez))
        hy = both(lambda h, e, r: h + 0.5 * (r - e), hy, ez, c_below(ez))
        hx_left, hy_up = c_left(hx), c_above(hy)
        if n == 2:
            edge = R2[pl.ds(1, 32, stride=8), :]

            def spread(idx):
                parts = [lane_gather(edge[8 * r : 8 * r + 8, :], idx) for r in range(4)]
                return jnp.concatenate(parts, axis=0)

            w1 = tuple(spread(t16 + 16 * h) for h in range(2))
            w2 = tuple(spread(jnp.where(t16 == 15, 48, 32) + 2 * (lane >> 4) + h) for h in range(2))
            hy = (hy[0], jnp.where(rows_in[1] == 15, w1[1], hy[1]))
            hx = tuple(jnp.where(col_in == 15, w2[h], hx[h]) for h in range(2))
            hy_up = (jnp.where(rows_in[0] == 0, w1[0], hy_up[0]), hy_up[1])
            hx_left = tuple(jnp.where(col_in == 0, w2[h], hx_left[h]) for h in range(2))
        drive = []
        for h in range(2):
            total = jnp.zeros((32, 128), f32)
            for k in range(4):
                total = total + jnp.where(
                    (tile32 == src_tile[k]) & (lane32 + 128 * h == src_cell[k]), WAVE[n, k], 0.0
                )
            drive.append(total)
        new = both(
            lambda d, e, g, y, yu, x, xl, s: d * e + g * ((y - yu) - (x - xl)) + s,
            damp, ez, gain, hy, hy_up, hx, hx_left, tuple(drive),
        )
        for m in range(3):
            share = (m + 1) / 3.0
            for h in range(2):
                CO[1 + m, pl.ds(32 * h, 32), :] = f_rim[h] * ((1.0 - share) * ez[h] + share * new[h])
        lax.fori_loop(0, 3, substeps, 0)
        for tg in range(4):
            means(tg)
        if n == 0:
            received(1, 2).wait()
        if n < 2:
            rim = R2[pl.ds(0, 32, stride=8), :]
            out = []
            for h in range(2):
                r = 2 * (lane >> 4) + h
                slot = jnp.where(
                    r == 0, t16, jnp.where(r == 15, 16 + t16, jnp.where(t16 == 0, 32 + r, 48 + r))
                )
                slot = (slot & 63) + 64 * n
                parts = [lane_gather(rim[8 * q : 8 * q + 8, :], slot) for q in range(4)]
                out.append(jnp.where(frame[h], jnp.concatenate(parts, axis=0), new[h]))
            new = tuple(out)
        ez = both(lambda m, x, y: jnp.where(m, x, y), mid, (CO[5, pl.ds(0, 32), :], CO[5, pl.ds(32, 32), :]), new)
        picked = jnp.zeros((8, 128), f32)
        for h in range(2):
            for q in range(4):
                got = lane_gather(ez[h][8 * q : 8 * q + 8, :], r_idx)
                picked = picked + jnp.where((r_tile == sub + 8 * q) & (r_half == h), got, 0.0)
        TS[pl.ds(n, 1), :] = jnp.sum(picked, axis=0, keepdims=True)

    for d in range(1, NB):
        n = lax.rem(b + d, NB)
        pltpu.make_async_remote_copy(
            src_ref=TS.at[pl.ds(0, 3), :],
            dst_ref=TB.at[pl.ds(pl.multiple_of(8 * b, 8), 3), :],
            send_sem=send_sem, recv_sem=recv_sem.at[4],
            device_id=dev(a, n), device_id_type=MESH,
        ).start()
    TB[pl.ds(pl.multiple_of(8 * b, 8), 3), :] = TS[pl.ds(0, 3), :]

    for k, field in enumerate((ez, hx, hy)):
        for h in range(2):
            O1[pl.ds(2 * k + h, 32, stride=8), :] = field[h]
    exchange(2, O1, RO1, 8, 6)

    from_cells(WE, FE)
    from_cells(WX, FX)
    seven = (NB - 1) * 3
    bytes_of(seven, recv_sem.at[4]).wait()
    for n in range(STEPS):
        TS2[pl.ds(n, 1), :] = jnp.sum(TB[pl.ds(n, 8, stride=8), :], axis=0, keepdims=True)
    exchange(3, TS2, TG, 8, 3, same=True)

    from_cells(WY, FY)
    received(2, 6).wait()

    def unpack(src, first, dst):
        for ci in range(4):
            for h in range(2):
                x = src[pl.ds(ci * 64 + first + h, 8, stride=8), :]
                dst[pl.ds(16 * ci + h, 8, stride=2), :] = swap_blocks(x, sub, lg)

    unpack(RO1, 0, ez_out)
    unpack(RO1, 2, hx_out)
    unpack(RO1, 4, hy_out)
    received(3, 3).wait()
    for n in range(STEPS):
        tr_out[pl.ds(n, 1), :] = jnp.sum(TG[pl.ds(n, 32, stride=8), :], axis=0, keepdims=True)

    bytes_of(224 + (NA - 1) * (9 + 2 + 6 + 3) + seven, send_sem).wait()


def finish(*refs):
    sources, outs, sems = refs[:7], refs[7:14], refs[14]
    copies = [pltpu.make_async_copy(x, y, sems.at[j]) for j, (x, y) in enumerate(zip(sources, outs))]
    for copy in copies:
        copy.start()
    for copy in copies:
        copy.wait()


def shards(
    coarse_ez, coarse_hx, coarse_hy, coarse_ids, mat_eps, mat_sig,
    fine_ez, fine_hx, fine_hy, fine_ids, boxes, src_cells, src_wave, rcv_cells,
):
    fine_shape = fine_ez.shape
    flat = (576, 128)
    anywhere = pl.BlockSpec(memory_space=pl.ANY)
    vmem = pl.BlockSpec(memory_space=pltpu.VMEM)
    shapes = ((64, 128),) * 3 + (flat,) * 3 + ((3, 128),)

    def v(*shape, dtype=f32):
        return pltpu.VMEM(shape, dtype)

    def dma(n):
        return pltpu.SemaphoreType.DMA((n,))

    outs = pl.pallas_call(
        kernel,
        name="nested",
        out_shape=tuple(pltpu.VMEM(shape, f32) for shape in shapes),
        in_specs=[anywhere] * 14,
        out_specs=(vmem,) * 7,
        scratch_shapes=[
            v(4, 80, 128), v(2, 80, 128), v(64, 128, dtype=i32), v(64, 128), v(80, 128), v(80, 128), v(4, 64, 128),
            v(512, 128), v(512, 128), v(256, 128), v(256, 128),
            v(256, 128), v(256, 128),
            v(8, 128), v(64, 128), v(8, 128), v(256, 128),
            v(576, 128, dtype=i32), v(584, 128), v(584, 128),
            v(584, 128), v(584, 128), v(584, 128),
            v(144, 128, dtype=i32), v(144, 128, dtype=i32), v(272, 128), v(6, 64, 128),
            v(4, 32, dtype=i32), pltpu.SMEM((1, 4), i32), pltpu.SMEM((3, 4), f32),
            v(1, 128, dtype=i32), v(1, 8), v(1, 8),
            v(2304, 128), dma(8), pltpu.SemaphoreType.DMA, pltpu.SemaphoreType.DMA, dma(5), pltpu.SemaphoreType.REGULAR,
        ],
        compiler_params=pltpu.CompilerParams(collective_id=0, has_side_effects=True),
    )(
        coarse_ez, coarse_hx, coarse_hy, coarse_ids,
        mat_eps.reshape(1, 8), mat_sig.reshape(1, 8),
        fine_ez.reshape(flat), fine_hx.reshape(flat), fine_hy.reshape(flat), fine_ids.reshape(flat),
        boxes.reshape(32, 4).T, src_cells.reshape(1, 4), src_wave, rcv_cells.reshape(1, 128),
    )
    outs = pl.pallas_call(
        finish,
        name="finish",
        out_shape=tuple(jax.ShapeDtypeStruct(shape, f32) for shape in shapes),
        in_specs=[vmem] * 7,
        out_specs=(anywhere,) * 7,
        scratch_shapes=[dma(7)],
    )(*(pltpu.with_memory_space_constraint(x, pltpu.VMEM) for x in outs))
    return tuple(outs[:3]) + tuple(x.reshape(fine_shape) for x in outs[3:6]) + (outs[6],)


def solution(mesh):
    coarse = P("gx", ("grp", "gy"))
    tiles = P(None, ("grp", "gy"), "gx", None)
    in_specs = (
        coarse, coarse, coarse, coarse, P(), P(), tiles, tiles, tiles, tiles,
        P("gx", ("grp", "gy"), None, None), P(), P(), P(),
    )
    out_specs = (coarse, coarse, coarse, tiles, tiles, tiles, P())
    return jax.shard_map(shards, mesh=mesh, in_specs=in_specs, out_specs=out_specs, check_vma=False)
```

```python
import functools

import jax
import jax.numpy as jnp
from jax import lax
from jax.experimental import pallas as pl
from jax.experimental.pallas import tpu as pltpu
from jax.sharding import PartitionSpec as P

MESH = pl.DeviceIdType.MESH
NA = 32
NB = 8
STEPS = 3
f32 = jnp.float32
i32 = jnp.int32


def lanes():
    return lax.broadcasted_iota(i32, (8, 128), 1)


def sublanes():
    return lax.broadcasted_iota(i32, (8, 128), 0)


def swap_blocks(x, turn, pick_rows, back):
    return lane_gather(jnp.take_along_axis(lane_gather(x, turn), pick_rows, axis=0), back)


def lane_gather(x, idx):
    return jnp.take_along_axis(x, idx, axis=1)


def div(x, n):
    return (x * ((1 << 20) // n + 1)) >> 20


FINE = 48


def sources_of_cells():
    need = [set() for _ in range(18)]
    back = [set() for _ in range(18)]
    for p in range(FINE):
        for q in range(FINE):
            u, g = 3 * (p % 6) + q % 3, (p * FINE + q) // 128
            need[u].add(g)
            back[g].add(u)
    return [sorted(x) for x in need], [sorted(x) for x in back]


NEED, BACK = sources_of_cells()


def pick(table, ids):
    bits = [(ids & (1 << k)) != 0 for k in range(3)]
    for bit in bits:
        table = [jnp.where(bit, table[i + 1], table[i]) for i in range(0, len(table), 2)]
    return table[0]


def step_tables(eps, sig, ratio):
    loss = sig / (eps * ratio)
    return (1.0 - loss) / (1.0 + loss), 0.5 / (eps * (1.0 + loss))


def kernel(
    ez_in, hx_in, hy_in, ids_in, eps_in, sig_in, fez_in, fhx_in, fhy_in, fids_in, box_in, src_in, wave_in, rcv_in,
    ez_out, hx_out, hy_out, fez_out, fhx_out, fhy_out, tr_out,
    HE, DG, IDS, PB, PEL, PER, E2, S1, R1, S2, R2, O1, RO1, TS, TB, TS2, TG,
    FI, FD, FG, WE, WX, WY, IDX, SEL, TAB, CO, BOX, SRC, WAVE, RCV, EPS, SIG,
    MANY, in_sem, halo_sem, send_sem, recv_sem, stage_sem, far_sem,
):
    FE, FX, FY = fez_out, fhx_out, fhy_out
    grp = lax.axis_index("grp")
    a = lax.axis_index("gx")
    gy = lax.axis_index("gy")
    b = grp * 4 + gy

    def dev(na, nb):
        return (nb // 4, na, nb % 4)

    am, ap = lax.rem(a + NA - 1, NA), lax.rem(a + 1, NA)
    bm, bp = lax.rem(b + NB - 1, NB), lax.rem(b + 1, NB)

    def bytes_of(rows, sem):
        return pltpu.make_async_copy(MANY.at[pl.ds(0, rows), :], MANY.at[pl.ds(0, rows), :], sem)

    loads = []
    for j, (source, dst) in enumerate((
        (ez_in, HE.at[0, pl.ds(8, 64), :]),
        (hx_in, HE.at[1, pl.ds(8, 64), :]),
        (hy_in, HE.at[2, pl.ds(8, 64), :]),
        (ids_in, IDS),
        (fids_in, FI),
        (fez_in, FE),
        (fhx_in, FX),
        (fhy_in, FY),
        (box_in, BOX),
        (eps_in, EPS),
        (sig_in, SIG),
        (rcv_in, RCV),
        (src_in, SRC),
        (wave_in, WAVE),
    )):
        copy = pltpu.make_async_copy(source, dst, in_sem.at[min(j // 4, 2) + max(j - 8, 0)])
        copy.start()
        loads.append(copy)

    barrier = pltpu.get_barrier_semaphore()

    def signal(na, nb):
        pl.semaphore_signal(barrier, inc=1, device_id=dev(na, nb), device_id_type=MESH)

    y, z = a // 8, lax.rem(a, 8)
    for d in (4, 3, 5, 2, 6):
        signal(y * 8 + lax.rem(z + d, 8), b)
    for na in (am, ap):
        for nb in (bm, b, bp):
            signal(na, nb)
    signal(a, bm)
    signal(a, bp)
    for d in (1, 7):
        signal(y * 8 + lax.rem(z + d, 8), b)
    y_peers = [lax.rem(y + d, 4) * 8 + z for d in range(1, 4)]
    for n in y_peers:
        signal(n, b)

    lane = lanes()
    sub = sublanes()
    lg = lane >> 4
    swap = (
        (((lg + sub) & 7) << 4) + (lane & 15),
        (sub - lg) & 7,
        (((sub - lg) & 7) << 4) + (lane & 15),
    )

    for g in range(18):
        pos = lane + 128 * g
        p = div(pos, 48)
        q = pos - 48 * p
        pb, j = div(p, 6), div(q, 3)
        IDX[pl.ds(8 * g, 8), :] = 16 * pb + j
        SEL[pl.ds(8 * g, 8), :] = 3 * (p - 6 * pb) + (q - 3 * j)
    cell_pos = 288 * (lane >> 4) + 3 * (lane & 15)

    def flat_rows(tg, g):
        return pl.ds(tg * 144 + g, 8, stride=18)

    def aligned(start, size):
        return pl.ds(start if isinstance(start, int) else pl.multiple_of(start, 8), size)

    def cell_rows(tg, u):
        return aligned(tg * 144 + 8 * u, 8)

    def each_pair(body):
        def pair(half, carry):
            for k in range(2):
                body(2 * half + k)
            return carry

        lax.fori_loop(0, 2, pair, 0)

    def to_cells(src, put):
        def body(tg):
            flat = [src[flat_rows(tg, g), :] for g in range(18)]
            for u in range(18):
                pos = cell_pos + (48 * (u // 3) + u % 3)
                idx, group = pos & 127, pos >> 7
                value = lane_gather(flat[NEED[u][0]], idx)
                for g in NEED[u][1:]:
                    value = jnp.where(group == g, lane_gather(flat[g], idx), value)
                put(tg, u, value)

        each_pair(body)

    def put_in(dst):
        def put(tg, u, value):
            dst[cell_rows(tg, u), :] = value

        return put

    def from_cells(src, dst):
        def body(tg):
            cells = [src[cell_rows(tg, u), :] for u in range(18)]
            for g in range(18):
                idx, group = IDX[pl.ds(8 * g, 8), :], SEL[pl.ds(8 * g, 8), :]
                value = lane_gather(cells[BACK[g][0]], idx)
                for u in BACK[g][1:]:
                    value = jnp.where(group == u, lane_gather(cells[u], idx), value)
                dst[flat_rows(tg, g), :] = value

        each_pair(body)

    bytes_of(4 * 64, in_sem.at[0]).wait()
    for copy in loads[8:]:
        copy.wait()
    HE[3, pl.ds(8, 64), :] = IDS[...].astype(f32)

    for v in range(8):
        ci, h = v // 2, v % 2
        for k in range(4):
            x = HE[k, pl.ds(8 + 16 * ci + h, 8, stride=2), :]
            S1[pl.ds(ci * 128 + 2 * k + h, 8, stride=16), :] = swap_blocks(x, *swap)
    row32 = lax.broadcasted_iota(i32, (32, 32), 0)
    col32 = lax.broadcasted_iota(i32, (32, 32), 1)
    lane32 = lax.broadcasted_iota(i32, (32, 128), 1)
    box_rows = jnp.zeros((32, 128), f32)
    for k in range(4):
        one = jnp.broadcast_to(BOX[pl.ds(k, 1), :], (32, 32)).astype(f32)
        value = jnp.sum(jnp.where(row32 == col32, one, 0.0), axis=1, keepdims=True)
        box_rows = jnp.where(lane32 == k, value, box_rows)
    S1[pl.ds(8, 32, stride=16), :] = box_rows

    lane64 = lax.broadcasted_iota(i32, (64, 128), 1)
    packed = jnp.zeros((64, 128), f32)
    for k in range(4):
        near = (lane64 - 8 * k) & 127
        x = HE[k, pl.ds(8, 64), :]
        packed = jnp.where((near < 3) | (near >= 125), pltpu.roll(x, 8 * k, 1) if k else x, packed)
    PB[...] = packed

    TAB[pl.ds(0, 8), :] = jnp.ones((8, 128), f32)
    TAB[pl.ds(8, 8), :] = jnp.zeros((8, 128), f32)
    TAB[pl.ds(0, 8), pl.ds(0, 8)] = jnp.broadcast_to(EPS[...], (8, 8))
    TAB[pl.ds(8, 8), pl.ds(0, 8)] = jnp.broadcast_to(SIG[...], (8, 8))
    eps, sig = TAB[pl.ds(0, 8), :], TAB[pl.ds(8, 8), :]
    for j, table in enumerate(step_tables(eps, sig, 1.0) + step_tables(eps, sig, 3.0)):
        for k in range(8):
            TAB[pl.ds(16 + 64 * j + 8 * k, 8), :] = jnp.broadcast_to(table[:, k : k + 1], (8, 128))

    def table(j):
        return [TAB[pl.ds(16 + 64 * j + 8 * k, 8), :] for k in range(8)]

    damp1, gain1, damp3, gain3 = (functools.partial(table, j) for j in range(4))


    def put_coef(tg, u, ids):
        FD[cell_rows(tg, u), :] = pick(damp3(), ids)
        FG[cell_rows(tg, u), :] = pick(gain3(), ids)

    pl.semaphore_wait(barrier, 6 + 2 + 7 + 3)
    for n in y_peers:
        pl.semaphore_signal(stage_sem, inc=1, device_id=dev(n, b), device_id_type=MESH)

    def halo(src, dst, na, nb):
        copy = pltpu.make_async_remote_copy(
            src_ref=src, dst_ref=dst, send_sem=send_sem, recv_sem=halo_sem,
            device_id=dev(na, nb), device_id_type=MESH,
        )
        copy.start()

    halo(HE.at[:, pl.ds(64, 8), :], HE.at[:, pl.ds(0, 8), :], ap, b)
    halo(HE.at[:, pl.ds(8, 8), :], HE.at[:, pl.ds(72, 8), :], am, b)
    halo(PB, PEL.at[pl.ds(8, 64), :], a, bp)
    halo(PB, PER.at[pl.ds(8, 64), :], a, bm)
    halo(PB.at[pl.ds(56, 8), :], PEL.at[pl.ds(0, 8), :], ap, bp)
    halo(PB.at[pl.ds(56, 8), :], PER.at[pl.ds(0, 8), :], ap, bm)
    halo(PB.at[pl.ds(0, 8), :], PEL.at[pl.ds(72, 8), :], am, bp)
    halo(PB.at[pl.ds(0, 8), :], PER.at[pl.ds(72, 8), :], am, bm)

    def ring(d, size):
        return min(d, size - d)

    offsets = sorted(
        ((dy, dz) for dy in range(4) for dz in range(8) if dy or dz), key=lambda o: -(ring(o[0], 4) + ring(o[1], 8))
    )
    peers = [lax.rem(a // 8 + dy, 4) * 8 + lax.rem(lax.rem(a, 8) + dz, 8) for dy, dz in offsets]

    def exchange(j, src, dst, slot, rows, same=False):
        own = pl.multiple_of(a * slot, slot)
        for n in peers:
            pltpu.make_async_remote_copy(
                src_ref=src.at[pl.ds(0 if same else pl.multiple_of(n * slot, slot), rows), :],
                dst_ref=dst.at[pl.ds(own, rows), :],
                send_sem=send_sem, recv_sem=recv_sem.at[j],
                device_id=dev(n, b), device_id_type=MESH,
            ).start()
        dst[pl.ds(own, rows), :] = src[pl.ds(0 if same else own, rows), :]

    def received(j, rows):
        return bytes_of((NA - 1) * rows, recv_sem.at[j])

    bytes_of(4 * 576, in_sem.at[1]).wait()
    to_cells(FI, put_coef)
    pl.semaphore_wait(stage_sem, 3)
    exchange(0, S1, R1, 16, 9)

    def tell(j, d):
        for n in (lax.rem(b + NB - d, NB), lax.rem(b + d, NB)):
            pl.semaphore_signal(far_sem.at[j], inc=1, device_id=dev(a, n), device_id_type=MESH)

    tell(0, 1)
    to_cells(FE, put_in(WE))

    def coef_rows(ids):
        ids = ids.astype(i32)
        return pick(damp1(), ids), pick(gain1(), ids)

    for r in range(1, 9):
        DG[0, pl.ds(8 * r, 8), :], DG[1, pl.ds(8 * r, 8), :] = coef_rows(HE[3, pl.ds(8 * r, 8), :])
    bytes_of(2 * 32 + 2 * 64 + 4 * 8, halo_sem).wait()
    for r in (0, 9):
        DG[0, pl.ds(8 * r, 8), :], DG[1, pl.ds(8 * r, 8), :] = coef_rows(HE[3, pl.ds(8 * r, 8), :])
    lane80 = lax.broadcasted_iota(i32, (80, 128), 1)
    row80 = lax.broadcasted_iota(i32, (80, 128), 0)
    row_g = row80 + (a * 64 - 8)
    col_m = lane80 + b * 128
    col_s = jnp.where(lane80 < 64, col_m + 128, col_m - 128)
    row_ok = (row_g >= 0) & (row_g < NA * 64)
    ok_m = jnp.where(row_ok, 1.0, 0.0)
    ok_s = jnp.where(row_ok & (col_s >= 0) & (col_s < NB * 128), 1.0, 0.0)

    def sides(k):
        left, right = PEL[...], PER[...]
        if k:
            left, right = pltpu.roll(left, 128 - 8 * k, 1), pltpu.roll(right, 128 - 8 * k, 1)
        return jnp.where(lane80 >= 125, left, jnp.where(lane80 < 3, right, 0.0))

    pair_ez, pair_hx, pair_hy = ((HE[k] * ok_m, sides(k) * ok_s) for k in range(3))

    ids_s = sides(3)
    sides_dg = [coef_rows(ids_s[8 * r : 8 * r + 8, :]) for r in range(10)]
    pair_damp, pair_gain = (
        (DG[k] * ok_m, jnp.concatenate([part[k] for part in sides_dg], axis=0) * ok_s) for k in range(2)
    )

    def right_of(x):
        m, s = pltpu.roll(x[0], 127, 1), pltpu.roll(x[1], 127, 1)
        return jnp.where(lane80 < 127, m, s), jnp.where(lane80 < 127, s, m)

    def left_of(x):
        m, s = pltpu.roll(x[0], 1, 1), pltpu.roll(x[1], 1, 1)
        return jnp.where(lane80 >= 1, m, s), jnp.where(lane80 >= 1, s, m)

    def below(x):
        return pltpu.roll(x[0], 79, 0), pltpu.roll(x[1], 79, 0)

    def above(x):
        return pltpu.roll(x[0], 1, 0), pltpu.roll(x[1], 1, 0)

    def both(fn, *pairs):
        return tuple(fn(*(p[i] for p in pairs)) for i in range(2))

    src_i = [SRC[0, k] >> 10 for k in range(4)]
    src_j = [SRC[0, k] & 1023 for k in range(4)]

    def h_step(ez, hx, hy):
        hx = both(lambda h, e, r, k: (h - 0.5 * (r - e)) * k, hx, ez, right_of(ez), (ok_m, ok_s))
        hy = both(lambda h, e, r, k: (h + 0.5 * (r - e)) * k, hy, ez, below(ez), (ok_m, ok_s))
        return hx, hy

    for n in range(2):
        pair_hx, pair_hy = h_step(pair_ez, pair_hx, pair_hy)
        drive = []
        for col in (col_m, col_s):
            total = jnp.zeros((80, 128), f32)
            for k in range(4):
                total = total + jnp.where((row_g == src_i[k]) & (col == src_j[k]), WAVE[n, k], 0.0)
            drive.append(total)
        pair_ez = both(
            lambda d, e, g, hy, hu, hx, hl, s: d * e + g * ((hy - hu) - (hx - hl)) + s,
            pair_damp, pair_ez, pair_gain, pair_hy, above(pair_hy), pair_hx, left_of(pair_hx), tuple(drive),
        )
        E2[n] = pair_ez[0][8:72, :]
    pair_hx, pair_hy = h_step(pair_ez, pair_hx, pair_hy)
    E2[2] = jnp.where((row80 & 15) == 8, above(pair_hy)[0], pair_hy[0])[8:72, :]
    E2[3] = jnp.where((lane80 & 15) == 0, left_of(pair_hx)[0], pair_hx[0])[8:72, :]

    e4, t16 = (lane >> 4) & 3, lane & 15
    frame_idx = jnp.where(
        e4 == 0, t16,
        jnp.where(e4 == 1, 112 + t16, jnp.where(e4 == 2, 16 * (t16 >> 1), 16 * (t16 >> 1) + 15)),
    )
    from_h1 = jnp.where(e4 == 0, 0, jnp.where(e4 == 1, 1, t16 & 1)) == 1

    for ci in range(4):
        got = []
        for k in range(4):
            halves = []
            for h in range(2):
                x = E2[k, pl.ds(16 * ci + h, 8, stride=2), :]
                halves.append(lane_gather(swap_blocks(x, *swap), frame_idx))
            got.append(jnp.where(from_h1, halves[1], halves[0]))
        S2[pl.ds(ci * 64, 8, stride=8), :] = jnp.where(lane < 64, got[0], got[1])
        S2[pl.ds(ci * 64 + 1, 8, stride=8), :] = jnp.where((lane & 63) < 32, got[2], got[3])

    exchange(1, S2, R2, 8, 2)

    pl.semaphore_wait(far_sem.at[0], 2)
    tell(1, 2)
    to_cells(FX, put_in(WX))
    to_cells(FY, put_in(WY))
    received(0, 9).wait()

    def from1(k):
        return tuple(R1[pl.ds(2 * k + h, 32, stride=16), :] for h in range(2))

    ez, hx, hy, ids_c = (from1(k) for k in range(4))

    def coef32(table, ids):
        parts = [pick(table, ids[8 * r : 8 * r + 8, :].astype(i32)) for r in range(4)]
        return jnp.concatenate(parts, axis=0)

    damp = tuple(coef32(damp1(), x) for x in ids_c)
    gain = tuple(coef32(gain1(), x) for x in ids_c)
    rows_in = tuple(2 * (lane32 >> 4) + h for h in range(2))
    col_in = lane32 & 15
    boxes = R1[pl.ds(8, 32, stride=16), :]
    lo_i, lo_j, n_i, n_j = (jnp.broadcast_to(boxes[:, k : k + 1], (32, 128)).astype(i32) for k in range(4))
    mid = tuple((r > lo_i) & (r < lo_i + n_i - 1) & (col_in > lo_j) & (col_in < lo_j + n_j - 1) for r in rows_in)
    inbox = tuple((r >= lo_i) & (r < lo_i + n_i) & (col_in >= lo_j) & (col_in < lo_j + n_j) for r in rows_in)
    f_mid = tuple(jnp.where(m, 1.0, 0.0) for m in mid)
    f_in = tuple(jnp.where(m, 1.0, 0.0) for m in inbox)
    f_rim = both(lambda x, y: x - y, f_in, f_mid)
    for h in range(2):
        CO[0, pl.ds(32 * h, 32), :] = 0.5 * f_in[h]
        CO[4, pl.ds(32 * h, 32), :] = f_mid[h]

    def co_rows(tg, h):
        return aligned(32 * h + 8 * tg, 8)

    def prepare(tg, carry):
        halves = [(2.0 * CO[0, co_rows(tg, h), :], CO[4, co_rows(tg, h), :]) for h in range(2)]
        for u in range(18):
            box, middle = halves[u // 9]
            rows = cell_rows(tg, u)
            WX[rows, :] = WX[rows, :] * box
            WY[rows, :] = WY[rows, :] * box
            FD[rows, :] = FD[rows, :] * middle
            FG[rows, :] = FG[rows, :] * middle
        return carry

    lax.fori_loop(0, 4, prepare, 0)

    def substeps(m, carry):
        for tg in range(4):
            substep(m, tg)
        return carry

    def substep(m, tg):
        half_box = [CO[0, co_rows(tg, h), :] for h in range(2)]
        rim = [CO[1 + m, co_rows(tg, h), :] for h in range(2)]
        e = [WE[cell_rows(tg, u), :] for u in range(18)]
        x, y = [None] * 18, [None] * 18

        def magnetic(p):
            for u in range(3 * p, 3 * p + 3):
                c = half_box[u // 9]
                after = e[u + 1] if u % 3 < 2 else pltpu.roll(e[u - 2], 127, 1)
                under = e[u + 3] if u < 15 else pltpu.roll(e[u - 15], 112, 1)
                x[u] = WX[cell_rows(tg, u), :] - c * (after - e[u])
                y[u] = WY[cell_rows(tg, u), :] + c * (under - e[u])
                WX[cell_rows(tg, u), :] = x[u]
                WY[cell_rows(tg, u), :] = y[u]

        def electric(p):
            for u in range(3 * p, 3 * p + 3):
                before = x[u - 1] if u % 3 else pltpu.roll(x[u + 2], 1, 1)
                over = y[u - 3] if u >= 3 else pltpu.roll(y[u + 15], 16, 1)
                curl = (y[u] - over) - (x[u] - before)
                WE[cell_rows(tg, u), :] = (
                    FD[cell_rows(tg, u), :] * e[u] + FG[cell_rows(tg, u), :] * curl + rim[u // 9]
                )

        magnetic(5)
        magnetic(0)
        for p in range(1, 5):
            magnetic(p)
            electric(p - 1)
        electric(4)
        electric(5)

    def means(tg):
        for h in range(2):
            part = [WE[cell_rows(tg, u), :] for u in range(9 * h, 9 * h + 9)]
            total = ((part[0] + part[1]) + (part[2] + part[3])) + ((part[4] + part[5]) + (part[6] + part[7])) + part[8]
            CO[5, co_rows(tg, h), :] = total * (1.0 / 9.0)

    edge_col = (col_in == 0) | (col_in == 15)
    frame = (edge_col | (rows_in[0] == 0), edge_col | (rows_in[1] == 15))
    tile32 = lax.broadcasted_iota(i32, (32, 128), 0)
    my_ci, my_cj = a // 8, lax.rem(a, 8)
    src_tile, src_cell = [], []
    for k in range(4):
        i, j = src_i[k], src_j[k]
        here = ((i & 63) >> 4 == my_ci) & ((j & 127) >> 4 == my_cj) & (j >> 7 == b)
        src_tile.append(jnp.where(here, i >> 6, -1))
        src_cell.append((i & 1) * 128 + ((i & 15) >> 1) * 16 + (j & 15))
    rcv = jnp.broadcast_to(RCV[...], (8, 128))
    ri, rj = rcv >> 10, rcv & 1023
    r_here = (((ri & 63) >> 4) == my_ci) & (((rj & 127) >> 4) == my_cj) & ((rj >> 7) == b)
    r_tile = jnp.where(r_here, ri >> 6, -1)
    r_idx, r_half = ((ri & 15) >> 1) * 16 + (rj & 15), ri & 1

    def c_right(x):
        return tuple(pltpu.roll(v, 127, 1) for v in x)

    def c_left(x):
        return tuple(pltpu.roll(v, 1, 1) for v in x)

    def c_below(x):
        return x[1], pltpu.roll(x[0], 112, 1)

    def c_above(x):
        return pltpu.roll(x[1], 16, 1), x[0]

    for n in range(STEPS):
        hx = both(lambda h, e, r: h - 0.5 * (r - e), hx, ez, c_right(ez))
        hy = both(lambda h, e, r: h + 0.5 * (r - e), hy, ez, c_below(ez))
        hx_left, hy_up = c_left(hx), c_above(hy)
        if n == 2:
            edge = R2[pl.ds(1, 32, stride=8), :]

            def spread(idx):
                parts = [lane_gather(edge[8 * r : 8 * r + 8, :], idx) for r in range(4)]
                return jnp.concatenate(parts, axis=0)

            w1 = tuple(spread(t16 + 16 * h) for h in range(2))
            w2 = tuple(spread(jnp.where(t16 == 15, 48, 32) + 2 * (lane >> 4) + h) for h in range(2))
            hy = (hy[0], jnp.where(rows_in[1] == 15, w1[1], hy[1]))
            hx = tuple(jnp.where(col_in == 15, w2[h], hx[h]) for h in range(2))
            hy_up = (jnp.where(rows_in[0] == 0, w1[0], hy_up[0]), hy_up[1])
            hx_left = tuple(jnp.where(col_in == 0, w2[h], hx_left[h]) for h in range(2))
        drive = []
        for h in range(2):
            total = jnp.zeros((32, 128), f32)
            for k in range(4):
                total = total + jnp.where(
                    (tile32 == src_tile[k]) & (lane32 + 128 * h == src_cell[k]), WAVE[n, k], 0.0
                )
            drive.append(total)
        new = both(
            lambda d, e, g, y, yu, x, xl, s: d * e + g * ((y - yu) - (x - xl)) + s,
            damp, ez, gain, hy, hy_up, hx, hx_left, tuple(drive),
        )
        for m in range(3):
            share = (m + 1) / 3.0
            for h in range(2):
                CO[1 + m, pl.ds(32 * h, 32), :] = f_rim[h] * ((1.0 - share) * ez[h] + share * new[h])
        for m in range(3):
            substeps(m, 0)
        for tg in range(4):
            means(tg)
        if n == 0:
            received(1, 2).wait()
        if n < 2:
            rim = R2[pl.ds(0, 32, stride=8), :]
            out = []
            for h in range(2):
                r = 2 * (lane >> 4) + h
                slot = jnp.where(
                    r == 0, t16, jnp.where(r == 15, 16 + t16, jnp.where(t16 == 0, 32 + r, 48 + r))
                )
                slot = (slot & 63) + 64 * n
                parts = [lane_gather(rim[8 * q : 8 * q + 8, :], slot) for q in range(4)]
                out.append(jnp.where(frame[h], jnp.concatenate(parts, axis=0), new[h]))
            new = tuple(out)
        ez = both(lambda m, x, y: jnp.where(m, x, y), mid, (CO[5, pl.ds(0, 32), :], CO[5, pl.ds(32, 32), :]), new)
        picked = jnp.zeros((8, 128), f32)
        for h in range(2):
            for q in range(4):
                got = lane_gather(ez[h][8 * q : 8 * q + 8, :], r_idx)
                picked = picked + jnp.where((r_tile == sub + 8 * q) & (r_half == h), got, 0.0)
        TS[pl.ds(n, 1), :] = jnp.sum(picked, axis=0, keepdims=True)

    pl.semaphore_wait(far_sem.at[1], 2)
    for d in range(1, NB):
        n = lax.rem(b + d, NB)
        pltpu.make_async_remote_copy(
            src_ref=TS.at[pl.ds(0, 3), :],
            dst_ref=TB.at[pl.ds(pl.multiple_of(8 * b, 8), 3), :],
            send_sem=send_sem, recv_sem=recv_sem.at[4],
            device_id=dev(a, n), device_id_type=MESH,
        ).start()
    TB[pl.ds(pl.multiple_of(8 * b, 8), 3), :] = TS[pl.ds(0, 3), :]

    for k, field in enumerate((ez, hx, hy)):
        for h in range(2):
            O1[pl.ds(2 * k + h, 32, stride=8), :] = field[h]
    exchange(2, O1, RO1, 8, 6)

    from_cells(WE, FE)
    from_cells(WX, FX)
    seven = (NB - 1) * 3
    bytes_of(seven, recv_sem.at[4]).wait()
    for n in range(STEPS):
        TS2[pl.ds(n, 1), :] = jnp.sum(TB[pl.ds(n, 8, stride=8), :], axis=0, keepdims=True)
    exchange(3, TS2, TG, 8, 3, same=True)

    from_cells(WY, FY)
    received(2, 6).wait()

    def unpack(src, first, dst):
        for ci in range(4):
            for h in range(2):
                x = src[pl.ds(ci * 64 + first + h, 8, stride=8), :]
                dst[pl.ds(16 * ci + h, 8, stride=2), :] = swap_blocks(x, *swap)

    unpack(RO1, 0, ez_out)
    unpack(RO1, 2, hx_out)
    unpack(RO1, 4, hy_out)
    received(3, 3).wait()
    for n in range(STEPS):
        tr_out[pl.ds(n, 1), :] = jnp.sum(TG[pl.ds(n, 32, stride=8), :], axis=0, keepdims=True)

    bytes_of(224 + (NA - 1) * (9 + 2 + 6 + 3) + seven, send_sem).wait()


def finish(*refs):
    sources, outs, sems = refs[:7], refs[7:14], refs[14]
    copies = [pltpu.make_async_copy(x, y, sems.at[j]) for j, (x, y) in enumerate(zip(sources, outs))]
    for copy in copies:
        copy.start()
    for copy in copies:
        copy.wait()


def shards(
    coarse_ez, coarse_hx, coarse_hy, coarse_ids, mat_eps, mat_sig,
    fine_ez, fine_hx, fine_hy, fine_ids, boxes, src_cells, src_wave, rcv_cells,
):
    fine_shape = fine_ez.shape
    flat = (576, 128)
    anywhere = pl.BlockSpec(memory_space=pl.ANY)
    vmem = pl.BlockSpec(memory_space=pltpu.VMEM)
    shapes = ((64, 128),) * 3 + (flat,) * 3 + ((3, 128),)

    def v(*shape, dtype=f32):
        return pltpu.VMEM(shape, dtype)

    def dma(n):
        return pltpu.SemaphoreType.DMA((n,))

    outs = pl.pallas_call(
        kernel,
        name="nested",
        out_shape=tuple(pltpu.VMEM(shape, f32) for shape in shapes),
        in_specs=[anywhere] * 14,
        out_specs=(vmem,) * 7,
        scratch_shapes=[
            v(4, 80, 128), v(2, 80, 128), v(64, 128, dtype=i32), v(64, 128), v(80, 128), v(80, 128), v(4, 64, 128),
            v(512, 128), v(512, 128), v(256, 128), v(256, 128),
            v(256, 128), v(256, 128),
            v(8, 128), v(64, 128), v(8, 128), v(256, 128),
            v(576, 128, dtype=i32), v(584, 128), v(584, 128),
            v(584, 128), v(584, 128), v(584, 128),
            v(144, 128, dtype=i32), v(144, 128, dtype=i32), v(272, 128), v(6, 64, 128),
            v(4, 32, dtype=i32), pltpu.SMEM((1, 4), i32), pltpu.SMEM((3, 4), f32),
            v(1, 128, dtype=i32), v(1, 8), v(1, 8),
            v(2304, 128), dma(8), pltpu.SemaphoreType.DMA, pltpu.SemaphoreType.DMA, dma(5), pltpu.SemaphoreType.REGULAR, pltpu.SemaphoreType.REGULAR((2,)),
        ],
        compiler_params=pltpu.CompilerParams(collective_id=0, has_side_effects=True),
    )(
        coarse_ez, coarse_hx, coarse_hy, coarse_ids,
        mat_eps.reshape(1, 8), mat_sig.reshape(1, 8),
        fine_ez.reshape(flat), fine_hx.reshape(flat), fine_hy.reshape(flat), fine_ids.reshape(flat),
        boxes.reshape(32, 4).T, src_cells.reshape(1, 4), src_wave, rcv_cells.reshape(1, 128),
    )
    outs = pl.pallas_call(
        finish,
        name="finish",
        out_shape=tuple(jax.ShapeDtypeStruct(shape, f32) for shape in shapes),
        in_specs=[vmem] * 7,
        out_specs=(anywhere,) * 7,
        scratch_shapes=[dma(7)],
    )(*(pltpu.with_memory_space_constraint(x, pltpu.VMEM) for x in outs))
    return tuple(outs[:3]) + tuple(x.reshape(fine_shape) for x in outs[3:6]) + (outs[6],)


def solution(mesh):
    coarse = P("gx", ("grp", "gy"))
    tiles = P(None, ("grp", "gy"), "gx", None)
    in_specs = (
        coarse, coarse, coarse, coarse, P(), P(), tiles, tiles, tiles, tiles,
        P("gx", ("grp", "gy"), None, None), P(), P(), P(),
    )
    out_specs = (coarse, coarse, coarse, tiles, tiles, tiles, P())
    return jax.shard_map(shards, mesh=mesh, in_specs=in_specs, out_specs=out_specs, check_vma=False)
```

```python
import functools

import jax
import jax.numpy as jnp
from jax import lax
from jax.experimental import pallas as pl
from jax.experimental.pallas import tpu as pltpu
from jax.sharding import PartitionSpec as P

MESH = pl.DeviceIdType.MESH
NA = 32
NB = 8
STEPS = 3
f32 = jnp.float32
i32 = jnp.int32


def lanes():
    return lax.broadcasted_iota(i32, (8, 128), 1)


def sublanes():
    return lax.broadcasted_iota(i32, (8, 128), 0)


def swap_blocks(x, turn, pick_rows, back):
    return lane_gather(jnp.take_along_axis(lane_gather(x, turn), pick_rows, axis=0), back)


def lane_gather(x, idx):
    return jnp.take_along_axis(x, idx, axis=1)


def div(x, n):
    return (x * ((1 << 20) // n + 1)) >> 20


FINE = 48


def sources_of_cells():
    need = [set() for _ in range(18)]
    back = [set() for _ in range(18)]
    for p in range(FINE):
        for q in range(FINE):
            u, g = 3 * (p % 6) + q % 3, (p * FINE + q) // 128
            need[u].add(g)
            back[g].add(u)
    return [sorted(x) for x in need], [sorted(x) for x in back]


NEED, BACK = sources_of_cells()


def pick(table, ids):
    bits = [(ids & (1 << k)) != 0 for k in range(3)]
    for bit in bits:
        table = [jnp.where(bit, table[i + 1], table[i]) for i in range(0, len(table), 2)]
    return table[0]


def step_tables(eps, sig, ratio):
    loss = sig / (eps * ratio)
    return (1.0 - loss) / (1.0 + loss), 0.5 / (eps * (1.0 + loss))


def kernel(
    ez_in, hx_in, hy_in, ids_in, eps_in, sig_in, fez_in, fhx_in, fhy_in, fids_in, box_in, src_in, wave_in, rcv_in,
    ez_out, hx_out, hy_out, fez_out, fhx_out, fhy_out, tr_out,
    HE, DG, IDS, PB, QL, QR, PEL, PER, E2, S1, R1, S2, R2, O1, RO1, TS, TB, TS2, TG,
    FI, FD, FG, WE, WX, WY, IDX, SEL, TAB, CO, BOX, SRC, WAVE, RCV, EPS, SIG,
    MANY, in_sem, halo_sem, send_sem, recv_sem, stage_sem, far_sem,
):
    FE, FX, FY = fez_out, fhx_out, fhy_out
    grp = lax.axis_index("grp")
    a = lax.axis_index("gx")
    gy = lax.axis_index("gy")
    b = grp * 4 + gy

    def dev(na, nb):
        return (nb // 4, na, nb % 4)

    am, ap = lax.rem(a + NA - 1, NA), lax.rem(a + 1, NA)
    bm, bp = lax.rem(b + NB - 1, NB), lax.rem(b + 1, NB)

    def bytes_of(rows, sem):
        return pltpu.make_async_copy(MANY.at[pl.ds(0, rows), :], MANY.at[pl.ds(0, rows), :], sem)

    loads = []
    for j, (source, dst) in enumerate((
        (ez_in, HE.at[0, pl.ds(8, 64), :]),
        (hx_in, HE.at[1, pl.ds(8, 64), :]),
        (hy_in, HE.at[2, pl.ds(8, 64), :]),
        (ids_in, IDS),
        (fids_in, FI),
        (fez_in, FE),
        (fhx_in, FX),
        (fhy_in, FY),
        (box_in, BOX),
        (eps_in, EPS),
        (sig_in, SIG),
        (rcv_in, RCV),
        (src_in, SRC),
        (wave_in, WAVE),
    )):
        copy = pltpu.make_async_copy(source, dst, in_sem.at[min(j // 4, 2) + max(j - 8, 0)])
        copy.start()
        loads.append(copy)

    barrier = pltpu.get_barrier_semaphore()

    def signal(na, nb):
        pl.semaphore_signal(barrier, inc=1, device_id=dev(na, nb), device_id_type=MESH)

    y, z = a // 8, lax.rem(a, 8)
    for d in (4, 3, 5, 2, 6):
        signal(y * 8 + lax.rem(z + d, 8), b)
    for na in (am, ap):
        for nb in (bm, b, bp):
            signal(na, nb)
    signal(a, bm)
    signal(a, bp)
    for d in (1, 7):
        signal(y * 8 + lax.rem(z + d, 8), b)
    y_peers = [lax.rem(y + d, 4) * 8 + z for d in range(1, 4)]
    for n in y_peers:
        signal(n, b)

    lane = lanes()
    sub = sublanes()
    lg = lane >> 4
    swap = (
        (((lg + sub) & 7) << 4) + (lane & 15),
        (sub - lg) & 7,
        (((sub - lg) & 7) << 4) + (lane & 15),
    )

    for g in range(18):
        pos = lane + 128 * g
        p = div(pos, 48)
        q = pos - 48 * p
        pb, j = div(p, 6), div(q, 3)
        IDX[pl.ds(8 * g, 8), :] = 16 * pb + j
        SEL[pl.ds(8 * g, 8), :] = 3 * (p - 6 * pb) + (q - 3 * j)
    cell_pos = 288 * (lane >> 4) + 3 * (lane & 15)

    def flat_rows(tg, g):
        return pl.ds(tg * 144 + g, 8, stride=18)

    def aligned(start, size):
        return pl.ds(start if isinstance(start, int) else pl.multiple_of(start, 8), size)

    def cell_rows(tg, u):
        return aligned(tg * 144 + 8 * u, 8)

    def each_pair(body):
        def pair(half, carry):
            for k in range(2):
                body(2 * half + k)
            return carry

        lax.fori_loop(0, 2, pair, 0)

    def to_cells(src, put):
        def body(tg):
            flat = [src[flat_rows(tg, g), :] for g in range(18)]
            for u in range(18):
                pos = cell_pos + (48 * (u // 3) + u % 3)
                idx, group = pos & 127, pos >> 7
                value = lane_gather(flat[NEED[u][0]], idx)
                for g in NEED[u][1:]:
                    value = jnp.where(group == g, lane_gather(flat[g], idx), value)
                put(tg, u, value)

        each_pair(body)

    def put_in(dst):
        def put(tg, u, value):
            dst[cell_rows(tg, u), :] = value

        return put

    def from_cells(src, dst):
        def body(tg):
            cells = [src[cell_rows(tg, u), :] for u in range(18)]
            for g in range(18):
                idx, group = IDX[pl.ds(8 * g, 8), :], SEL[pl.ds(8 * g, 8), :]
                value = lane_gather(cells[BACK[g][0]], idx)
                for u in BACK[g][1:]:
                    value = jnp.where(group == u, lane_gather(cells[u], idx), value)
                dst[flat_rows(tg, g), :] = value

        each_pair(body)

    bytes_of(4 * 64, in_sem.at[0]).wait()
    for copy in loads[8:]:
        copy.wait()
    HE[3, pl.ds(8, 64), :] = IDS[...].astype(f32)

    for v in range(8):
        ci, h = v // 2, v % 2
        for k in range(4):
            x = HE[k, pl.ds(8 + 16 * ci + h, 8, stride=2), :]
            S1[pl.ds(ci * 128 + 2 * k + h, 8, stride=16), :] = swap_blocks(x, *swap)
    row32 = lax.broadcasted_iota(i32, (32, 32), 0)
    col32 = lax.broadcasted_iota(i32, (32, 32), 1)
    lane32 = lax.broadcasted_iota(i32, (32, 128), 1)
    box_rows = jnp.zeros((32, 128), f32)
    for k in range(4):
        one = jnp.broadcast_to(BOX[pl.ds(k, 1), :], (32, 32)).astype(f32)
        value = jnp.sum(jnp.where(row32 == col32, one, 0.0), axis=1, keepdims=True)
        box_rows = jnp.where(lane32 == k, value, box_rows)
    S1[pl.ds(8, 32, stride=16), :] = box_rows

    lane64 = lax.broadcasted_iota(i32, (64, 128), 1)
    packed = jnp.zeros((64, 128), f32)
    for k in range(4):
        near = (lane64 - 8 * k) & 127
        x = HE[k, pl.ds(8, 64), :]
        packed = jnp.where((near < 3) | (near >= 125), pltpu.roll(x, 8 * k, 1) if k else x, packed)
    packed = jnp.where(lane64 < 29, packed, pltpu.roll(packed, 32, 1))
    quarter = lane64[0:16, :] >> 5
    small = packed[0:16, :]
    for k in range(1, 4):
        small = jnp.where(quarter == k, pltpu.roll(packed[16 * k : 16 * k + 16, :], 32 * k, 1), small)
    PB[...] = small

    TAB[pl.ds(0, 8), :] = jnp.ones((8, 128), f32)
    TAB[pl.ds(8, 8), :] = jnp.zeros((8, 128), f32)
    TAB[pl.ds(0, 8), pl.ds(0, 8)] = jnp.broadcast_to(EPS[...], (8, 8))
    TAB[pl.ds(8, 8), pl.ds(0, 8)] = jnp.broadcast_to(SIG[...], (8, 8))
    eps, sig = TAB[pl.ds(0, 8), :], TAB[pl.ds(8, 8), :]
    for j, table in enumerate(step_tables(eps, sig, 1.0) + step_tables(eps, sig, 3.0)):
        for k in range(8):
            TAB[pl.ds(16 + 64 * j + 8 * k, 8), :] = jnp.broadcast_to(table[:, k : k + 1], (8, 128))

    def table(j):
        return [TAB[pl.ds(16 + 64 * j + 8 * k, 8), :] for k in range(8)]

    damp1, gain1, damp3, gain3 = (functools.partial(table, j) for j in range(4))


    def put_coef(tg, u, ids):
        FD[cell_rows(tg, u), :] = pick(damp3(), ids)
        FG[cell_rows(tg, u), :] = pick(gain3(), ids)

    pl.semaphore_wait(barrier, 6 + 2 + 7 + 3)
    for n in y_peers:
        pl.semaphore_signal(stage_sem, inc=1, device_id=dev(n, b), device_id_type=MESH)

    def halo(src, dst, na, nb):
        copy = pltpu.make_async_remote_copy(
            src_ref=src, dst_ref=dst, send_sem=send_sem, recv_sem=halo_sem,
            device_id=dev(na, nb), device_id_type=MESH,
        )
        copy.start()

    halo(HE.at[:, pl.ds(64, 8), :], HE.at[:, pl.ds(0, 8), :], ap, b)
    halo(HE.at[:, pl.ds(8, 8), :], HE.at[:, pl.ds(72, 8), :], am, b)
    halo(PB, QL.at[pl.ds(8, 16), :], a, bp)
    halo(PB, QR.at[pl.ds(8, 16), :], a, bm)
    halo(PB.at[pl.ds(8, 8), :], QL.at[pl.ds(0, 8), :], ap, bp)
    halo(PB.at[pl.ds(8, 8), :], QR.at[pl.ds(0, 8), :], ap, bm)
    halo(PB.at[pl.ds(0, 8), :], QL.at[pl.ds(24, 8), :], am, bp)
    halo(PB.at[pl.ds(0, 8), :], QR.at[pl.ds(24, 8), :], am, bm)

    def ring(d, size):
        return min(d, size - d)

    offsets = sorted(
        ((dy, dz) for dy in range(4) for dz in range(8) if dy or dz), key=lambda o: -(ring(o[0], 4) + ring(o[1], 8))
    )
    peers = [lax.rem(a // 8 + dy, 4) * 8 + lax.rem(lax.rem(a, 8) + dz, 8) for dy, dz in offsets]

    def exchange(j, src, dst, slot, rows, same=False):
        own = pl.multiple_of(a * slot, slot)
        for n in peers:
            pltpu.make_async_remote_copy(
                src_ref=src.at[pl.ds(0 if same else pl.multiple_of(n * slot, slot), rows), :],
                dst_ref=dst.at[pl.ds(own, rows), :],
                send_sem=send_sem, recv_sem=recv_sem.at[j],
                device_id=dev(n, b), device_id_type=MESH,
            ).start()
        dst[pl.ds(own, rows), :] = src[pl.ds(0 if same else own, rows), :]

    def received(j, rows):
        return bytes_of((NA - 1) * rows, recv_sem.at[j])

    bytes_of(4 * 576, in_sem.at[1]).wait()
    to_cells(FI, put_coef)
    pl.semaphore_wait(stage_sem, 3)
    exchange(0, S1, R1, 16, 9)

    def tell(j, d):
        for n in (lax.rem(b + NB - d, NB), lax.rem(b + d, NB)):
            pl.semaphore_signal(far_sem.at[j], inc=1, device_id=dev(a, n), device_id_type=MESH)

    tell(0, 1)
    to_cells(FE, put_in(WE))

    def coef_rows(ids):
        ids = ids.astype(i32)
        return pick(damp1(), ids), pick(gain1(), ids)

    for r in range(1, 9):
        DG[0, pl.ds(8 * r, 8), :], DG[1, pl.ds(8 * r, 8), :] = coef_rows(HE[3, pl.ds(8 * r, 8), :])
    bytes_of(2 * 32 + 2 * 16 + 4 * 8, halo_sem).wait()
    for small, wide in ((QL, PEL), (QR, PER)):
        wide[pl.ds(0, 8), :] = pltpu.roll(small[pl.ds(0, 8), :], 32, 1)
        wide[pl.ds(72, 8), :] = small[pl.ds(24, 8), :]
        for k in range(4):
            x = small[pl.ds(8, 16), :]
            wide[pl.ds(8 + 16 * k, 16), :] = pltpu.roll(x, 128 - 32 * k, 1) if k else x
    for r in (0, 9):
        DG[0, pl.ds(8 * r, 8), :], DG[1, pl.ds(8 * r, 8), :] = coef_rows(HE[3, pl.ds(8 * r, 8), :])
    lane80 = lax.broadcasted_iota(i32, (80, 128), 1)
    row80 = lax.broadcasted_iota(i32, (80, 128), 0)
    row_g = row80 + (a * 64 - 8)
    col_m = lane80 + b * 128
    col_s = jnp.where(lane80 < 64, col_m + 128, col_m - 128)
    row_ok = (row_g >= 0) & (row_g < NA * 64)
    ok_m = jnp.where(row_ok, 1.0, 0.0)
    ok_s = jnp.where(row_ok & (col_s >= 0) & (col_s < NB * 128), 1.0, 0.0)

    def sides(k):
        left, right = PEL[...], PER[...]
        if k:
            left, right = pltpu.roll(left, 128 - 8 * k, 1), pltpu.roll(right, 128 - 8 * k, 1)
        else:
            left = pltpu.roll(left, 96, 1)
        return jnp.where(lane80 >= 125, left, jnp.where(lane80 < 3, right, 0.0))

    pair_ez, pair_hx, pair_hy = ((HE[k] * ok_m, sides(k) * ok_s) for k in range(3))

    ids_s = sides(3)
    sides_dg = [coef_rows(ids_s[8 * r : 8 * r + 8, :]) for r in range(10)]
    pair_damp, pair_gain = (
        (DG[k] * ok_m, jnp.concatenate([part[k] for part in sides_dg], axis=0) * ok_s) for k in range(2)
    )

    def right_of(x):
        m, s = pltpu.roll(x[0], 127, 1), pltpu.roll(x[1], 127, 1)
        return jnp.where(lane80 < 127, m, s), jnp.where(lane80 < 127, s, m)

    def left_of(x):
        m, s = pltpu.roll(x[0], 1, 1), pltpu.roll(x[1], 1, 1)
        return jnp.where(lane80 >= 1, m, s), jnp.where(lane80 >= 1, s, m)

    def below(x):
        return pltpu.roll(x[0], 79, 0), pltpu.roll(x[1], 79, 0)

    def above(x):
        return pltpu.roll(x[0], 1, 0), pltpu.roll(x[1], 1, 0)

    def both(fn, *pairs):
        return tuple(fn(*(p[i] for p in pairs)) for i in range(2))

    src_i = [SRC[0, k] >> 10 for k in range(4)]
    src_j = [SRC[0, k] & 1023 for k in range(4)]

    def h_step(ez, hx, hy):
        hx = both(lambda h, e, r, k: (h - 0.5 * (r - e)) * k, hx, ez, right_of(ez), (ok_m, ok_s))
        hy = both(lambda h, e, r, k: (h + 0.5 * (r - e)) * k, hy, ez, below(ez), (ok_m, ok_s))
        return hx, hy

    for n in range(2):
        pair_hx, pair_hy = h_step(pair_ez, pair_hx, pair_hy)
        drive = []
        for col in (col_m, col_s):
            total = jnp.zeros((80, 128), f32)
            for k in range(4):
                total = total + jnp.where((row_g == src_i[k]) & (col == src_j[k]), WAVE[n, k], 0.0)
            drive.append(total)
        pair_ez = both(
            lambda d, e, g, hy, hu, hx, hl, s: d * e + g * ((hy - hu) - (hx - hl)) + s,
            pair_damp, pair_ez, pair_gain, pair_hy, above(pair_hy), pair_hx, left_of(pair_hx), tuple(drive),
        )
        E2[n] = pair_ez[0][8:72, :]
    pair_hx, pair_hy = h_step(pair_ez, pair_hx, pair_hy)
    E2[2] = jnp.where((row80 & 15) == 8, above(pair_hy)[0], pair_hy[0])[8:72, :]
    E2[3] = jnp.where((lane80 & 15) == 0, left_of(pair_hx)[0], pair_hx[0])[8:72, :]

    e4, t16 = (lane >> 4) & 3, lane & 15
    frame_idx = jnp.where(
        e4 == 0, t16,
        jnp.where(e4 == 1, 112 + t16, jnp.where(e4 == 2, 16 * (t16 >> 1), 16 * (t16 >> 1) + 15)),
    )
    from_h1 = jnp.where(e4 == 0, 0, jnp.where(e4 == 1, 1, t16 & 1)) == 1

    for ci in range(4):
        got = []
        for k in range(4):
            halves = []
            for h in range(2):
                x = E2[k, pl.ds(16 * ci + h, 8, stride=2), :]
                halves.append(lane_gather(swap_blocks(x, *swap), frame_idx))
            got.append(jnp.where(from_h1, halves[1], halves[0]))
        S2[pl.ds(ci * 64, 8, stride=8), :] = jnp.where(lane < 64, got[0], got[1])
        S2[pl.ds(ci * 64 + 1, 8, stride=8), :] = jnp.where((lane & 63) < 32, got[2], got[3])

    exchange(1, S2, R2, 8, 2)

    pl.semaphore_wait(far_sem.at[0], 2)
    tell(1, 2)
    to_cells(FX, put_in(WX))
    to_cells(FY, put_in(WY))
    received(0, 9).wait()

    def from1(k):
        return tuple(R1[pl.ds(2 * k + h, 32, stride=16), :] for h in range(2))

    ez, hx, hy, ids_c = (from1(k) for k in range(4))

    def coef32(table, ids):
        parts = [pick(table, ids[8 * r : 8 * r + 8, :].astype(i32)) for r in range(4)]
        return jnp.concatenate(parts, axis=0)

    damp = tuple(coef32(damp1(), x) for x in ids_c)
    gain = tuple(coef32(gain1(), x) for x in ids_c)
    rows_in = tuple(2 * (lane32 >> 4) + h for h in range(2))
    col_in = lane32 & 15
    boxes = R1[pl.ds(8, 32, stride=16), :]
    lo_i, lo_j, n_i, n_j = (jnp.broadcast_to(boxes[:, k : k + 1], (32, 128)).astype(i32) for k in range(4))
    mid = tuple((r > lo_i) & (r < lo_i + n_i - 1) & (col_in > lo_j) & (col_in < lo_j + n_j - 1) for r in rows_in)
    inbox = tuple((r >= lo_i) & (r < lo_i + n_i) & (col_in >= lo_j) & (col_in < lo_j + n_j) for r in rows_in)
    f_mid = tuple(jnp.where(m, 1.0, 0.0) for m in mid)
    f_in = tuple(jnp.where(m, 1.0, 0.0) for m in inbox)
    f_rim = both(lambda x, y: x - y, f_in, f_mid)
    for h in range(2):
        CO[0, pl.ds(32 * h, 32), :] = 0.5 * f_in[h]
        CO[4, pl.ds(32 * h, 32), :] = f_mid[h]

    def co_rows(tg, h):
        return aligned(32 * h + 8 * tg, 8)

    def prepare(tg, carry):
        halves = [(2.0 * CO[0, co_rows(tg, h), :], CO[4, co_rows(tg, h), :]) for h in range(2)]
        for u in range(18):
            box, middle = halves[u // 9]
            rows = cell_rows(tg, u)
            WX[rows, :] = WX[rows, :] * box
            WY[rows, :] = WY[rows, :] * box
            FD[rows, :] = FD[rows, :] * middle
            FG[rows, :] = FG[rows, :] * middle
        return carry

    lax.fori_loop(0, 4, prepare, 0)

    def substeps(m, carry):
        for tg in range(4):
            substep(m, tg)
        return carry

    def substep(m, tg):
        half_box = [CO[0, co_rows(tg, h), :] for h in range(2)]
        rim = [CO[1 + m, co_rows(tg, h), :] for h in range(2)]
        e = [WE[cell_rows(tg, u), :] for u in range(18)]
        x, y = [None] * 18, [None] * 18

        def magnetic(p):
            for u in range(3 * p, 3 * p + 3):
                c = half_box[u // 9]
                after = e[u + 1] if u % 3 < 2 else pltpu.roll(e[u - 2], 127, 1)
                under = e[u + 3] if u < 15 else pltpu.roll(e[u - 15], 112, 1)
                x[u] = WX[cell_rows(tg, u), :] - c * (after - e[u])
                y[u] = WY[cell_rows(tg, u), :] + c * (under - e[u])
                WX[cell_rows(tg, u), :] = x[u]
                WY[cell_rows(tg, u), :] = y[u]

        def electric(p):
            for u in range(3 * p, 3 * p + 3):
                before = x[u - 1] if u % 3 else pltpu.roll(x[u + 2], 1, 1)
                over = y[u - 3] if u >= 3 else pltpu.roll(y[u + 15], 16, 1)
                curl = (y[u] - over) - (x[u] - before)
                WE[cell_rows(tg, u), :] = (
                    FD[cell_rows(tg, u), :] * e[u] + FG[cell_rows(tg, u), :] * curl + rim[u // 9]
                )

        magnetic(5)
        magnetic(0)
        for p in range(1, 5):
            magnetic(p)
            electric(p - 1)
        electric(4)
        electric(5)

    def means(tg):
        for h in range(2):
            part = [WE[cell_rows(tg, u), :] for u in range(9 * h, 9 * h + 9)]
            total = ((part[0] + part[1]) + (part[2] + part[3])) + ((part[4] + part[5]) + (part[6] + part[7])) + part[8]
            CO[5, co_rows(tg, h), :] = total * (1.0 / 9.0)

    edge_col = (col_in == 0) | (col_in == 15)
    frame = (edge_col | (rows_in[0] == 0), edge_col | (rows_in[1] == 15))
    tile32 = lax.broadcasted_iota(i32, (32, 128), 0)
    my_ci, my_cj = a // 8, lax.rem(a, 8)
    src_tile, src_cell = [], []
    for k in range(4):
        i, j = src_i[k], src_j[k]
        here = ((i & 63) >> 4 == my_ci) & ((j & 127) >> 4 == my_cj) & (j >> 7 == b)
        src_tile.append(jnp.where(here, i >> 6, -1))
        src_cell.append((i & 1) * 128 + ((i & 15) >> 1) * 16 + (j & 15))
    rcv = jnp.broadcast_to(RCV[...], (8, 128))
    ri, rj = rcv >> 10, rcv & 1023
    r_here = (((ri & 63) >> 4) == my_ci) & (((rj & 127) >> 4) == my_cj) & ((rj >> 7) == b)
    r_tile = jnp.where(r_here, ri >> 6, -1)
    r_idx, r_half = ((ri & 15) >> 1) * 16 + (rj & 15), ri & 1

    def c_right(x):
        return tuple(pltpu.roll(v, 127, 1) for v in x)

    def c_left(x):
        return tuple(pltpu.roll(v, 1, 1) for v in x)

    def c_below(x):
        return x[1], pltpu.roll(x[0], 112, 1)

    def c_above(x):
        return pltpu.roll(x[1], 16, 1), x[0]

    for n in range(STEPS):
        hx = both(lambda h, e, r: h - 0.5 * (r - e), hx, ez, c_right(ez))
        hy = both(lambda h, e, r: h + 0.5 * (r - e), hy, ez, c_below(ez))
        hx_left, hy_up = c_left(hx), c_above(hy)
        if n == 2:
            edge = R2[pl.ds(1, 32, stride=8), :]

            def spread(idx):
                parts = [lane_gather(edge[8 * r : 8 * r + 8, :], idx) for r in range(4)]
                return jnp.concatenate(parts, axis=0)

            w1 = tuple(spread(t16 + 16 * h) for h in range(2))
            w2 = tuple(spread(jnp.where(t16 == 15, 48, 32) + 2 * (lane >> 4) + h) for h in range(2))
            hy = (hy[0], jnp.where(rows_in[1] == 15, w1[1], hy[1]))
            hx = tuple(jnp.where(col_in == 15, w2[h], hx[h]) for h in range(2))
            hy_up = (jnp.where(rows_in[0] == 0, w1[0], hy_up[0]), hy_up[1])
            hx_left = tuple(jnp.where(col_in == 0, w2[h], hx_left[h]) for h in range(2))
        drive = []
        for h in range(2):
            total = jnp.zeros((32, 128), f32)
            for k in range(4):
                total = total + jnp.where(
                    (tile32 == src_tile[k]) & (lane32 + 128 * h == src_cell[k]), WAVE[n, k], 0.0
                )
            drive.append(total)
        new = both(
            lambda d, e, g, y, yu, x, xl, s: d * e + g * ((y - yu) - (x - xl)) + s,
            damp, ez, gain, hy, hy_up, hx, hx_left, tuple(drive),
        )
        for m in range(3):
            share = (m + 1) / 3.0
            for h in range(2):
                CO[1 + m, pl.ds(32 * h, 32), :] = f_rim[h] * ((1.0 - share) * ez[h] + share * new[h])
        for m in range(3):
            substeps(m, 0)
        for tg in range(4):
            means(tg)
        if n == 0:
            received(1, 2).wait()
        if n < 2:
            rim = R2[pl.ds(0, 32, stride=8), :]
            out = []
            for h in range(2):
                r = 2 * (lane >> 4) + h
                slot = jnp.where(
                    r == 0, t16, jnp.where(r == 15, 16 + t16, jnp.where(t16 == 0, 32 + r, 48 + r))
                )
                slot = (slot & 63) + 64 * n
                parts = [lane_gather(rim[8 * q : 8 * q + 8, :], slot) for q in range(4)]
                out.append(jnp.where(frame[h], jnp.concatenate(parts, axis=0), new[h]))
            new = tuple(out)
        ez = both(lambda m, x, y: jnp.where(m, x, y), mid, (CO[5, pl.ds(0, 32), :], CO[5, pl.ds(32, 32), :]), new)
        picked = jnp.zeros((8, 128), f32)
        for h in range(2):
            for q in range(4):
                got = lane_gather(ez[h][8 * q : 8 * q + 8, :], r_idx)
                picked = picked + jnp.where((r_tile == sub + 8 * q) & (r_half == h), got, 0.0)
        TS[pl.ds(n, 1), :] = jnp.sum(picked, axis=0, keepdims=True)

    pl.semaphore_wait(far_sem.at[1], 2)
    for d in range(1, NB):
        n = lax.rem(b + d, NB)
        pltpu.make_async_remote_copy(
            src_ref=TS.at[pl.ds(0, 3), :],
            dst_ref=TB.at[pl.ds(pl.multiple_of(8 * b, 8), 3), :],
            send_sem=send_sem, recv_sem=recv_sem.at[4],
            device_id=dev(a, n), device_id_type=MESH,
        ).start()
    TB[pl.ds(pl.multiple_of(8 * b, 8), 3), :] = TS[pl.ds(0, 3), :]

    for k, field in enumerate((ez, hx, hy)):
        for h in range(2):
            O1[pl.ds(2 * k + h, 32, stride=8), :] = field[h]
    exchange(2, O1, RO1, 8, 6)

    from_cells(WE, FE)
    from_cells(WX, FX)
    seven = (NB - 1) * 3
    bytes_of(seven, recv_sem.at[4]).wait()
    for n in range(STEPS):
        TS2[pl.ds(n, 1), :] = jnp.sum(TB[pl.ds(n, 8, stride=8), :], axis=0, keepdims=True)
    exchange(3, TS2, TG, 8, 3, same=True)

    from_cells(WY, FY)
    received(2, 6).wait()

    def unpack(src, first, dst):
        for ci in range(4):
            for h in range(2):
                x = src[pl.ds(ci * 64 + first + h, 8, stride=8), :]
                dst[pl.ds(16 * ci + h, 8, stride=2), :] = swap_blocks(x, *swap)

    unpack(RO1, 0, ez_out)
    unpack(RO1, 2, hx_out)
    unpack(RO1, 4, hy_out)
    received(3, 3).wait()
    for n in range(STEPS):
        tr_out[pl.ds(n, 1), :] = jnp.sum(TG[pl.ds(n, 32, stride=8), :], axis=0, keepdims=True)

    bytes_of(128 + (NA - 1) * (9 + 2 + 6 + 3) + seven, send_sem).wait()


def finish(*refs):
    sources, outs, sems = refs[:7], refs[7:14], refs[14]
    copies = [pltpu.make_async_copy(x, y, sems.at[j]) for j, (x, y) in enumerate(zip(sources, outs))]
    for copy in copies:
        copy.start()
    for copy in copies:
        copy.wait()


def shards(
    coarse_ez, coarse_hx, coarse_hy, coarse_ids, mat_eps, mat_sig,
    fine_ez, fine_hx, fine_hy, fine_ids, boxes, src_cells, src_wave, rcv_cells,
):
    fine_shape = fine_ez.shape
    flat = (576, 128)
    anywhere = pl.BlockSpec(memory_space=pl.ANY)
    vmem = pl.BlockSpec(memory_space=pltpu.VMEM)
    shapes = ((64, 128),) * 3 + (flat,) * 3 + ((3, 128),)

    def v(*shape, dtype=f32):
        return pltpu.VMEM(shape, dtype)

    def dma(n):
        return pltpu.SemaphoreType.DMA((n,))

    outs = pl.pallas_call(
        kernel,
        name="nested",
        out_shape=tuple(pltpu.VMEM(shape, f32) for shape in shapes),
        in_specs=[anywhere] * 14,
        out_specs=(vmem,) * 7,
        scratch_shapes=[
            v(4, 80, 128), v(2, 80, 128), v(64, 128, dtype=i32),
            v(16, 128), v(32, 128), v(32, 128), v(80, 128), v(80, 128), v(4, 64, 128),
            v(512, 128), v(512, 128), v(256, 128), v(256, 128),
            v(256, 128), v(256, 128),
            v(8, 128), v(64, 128), v(8, 128), v(256, 128),
            v(576, 128, dtype=i32), v(584, 128), v(584, 128),
            v(584, 128), v(584, 128), v(584, 128),
            v(144, 128, dtype=i32), v(144, 128, dtype=i32), v(272, 128), v(6, 64, 128),
            v(4, 32, dtype=i32), pltpu.SMEM((1, 4), i32), pltpu.SMEM((3, 4), f32),
            v(1, 128, dtype=i32), v(1, 8), v(1, 8),
            v(2304, 128), dma(8), pltpu.SemaphoreType.DMA, pltpu.SemaphoreType.DMA, dma(5), pltpu.SemaphoreType.REGULAR, pltpu.SemaphoreType.REGULAR((2,)),
        ],
        compiler_params=pltpu.CompilerParams(collective_id=0, has_side_effects=True),
    )(
        coarse_ez, coarse_hx, coarse_hy, coarse_ids,
        mat_eps.reshape(1, 8), mat_sig.reshape(1, 8),
        fine_ez.reshape(flat), fine_hx.reshape(flat), fine_hy.reshape(flat), fine_ids.reshape(flat),
        boxes.reshape(32, 4).T, src_cells.reshape(1, 4), src_wave, rcv_cells.reshape(1, 128),
    )
    outs = pl.pallas_call(
        finish,
        name="finish",
        out_shape=tuple(jax.ShapeDtypeStruct(shape, f32) for shape in shapes),
        in_specs=[vmem] * 7,
        out_specs=(anywhere,) * 7,
        scratch_shapes=[dma(7)],
    )(*(pltpu.with_memory_space_constraint(x, pltpu.VMEM) for x in outs))
    return tuple(outs[:3]) + tuple(x.reshape(fine_shape) for x in outs[3:6]) + (outs[6],)


def solution(mesh):
    coarse = P("gx", ("grp", "gy"))
    tiles = P(None, ("grp", "gy"), "gx", None)
    in_specs = (
        coarse, coarse, coarse, coarse, P(), P(), tiles, tiles, tiles, tiles,
        P("gx", ("grp", "gy"), None, None), P(), P(), P(),
    )
    out_specs = (coarse, coarse, coarse, tiles, tiles, tiles, P())
    return jax.shard_map(shards, mesh=mesh, in_specs=in_specs, out_specs=out_specs, check_vma=False)
```
